32 devices in a mesh: runs: 2 (over y), gx: 4 (over z), gy: 2 (over x), gz: 2 (over core).
Axes of the slice: x: 2, y: 2, z: 4, core: 2. Of those that a mesh axis runs over, the one named last changes fastest.
Arguments:
- positions: float32 [3, 8, 4096], P(None, None, ('runs', 'gx', 'gy', 'gz')), parts along dimension 2, as said below
- velocities: float32 [3, 8, 4096], P(None, None, ('runs', 'gx', 'gy', 'gz')), parts along dimension 2, may hold values from -5 to 5
- send_list: int32 [5696], P(('runs', 'gx', 'gy', 'gz')), parts along dimension 0, may hold values from 0 to 127, as said below
- pair_list: int32 [2, 57344], P(None, ('runs', 'gx', 'gy', 'gz')), parts along dimension 1, may hold values from 0 to 306, as said below
- constraint_flags: int32 [7, 4096], P(None, ('runs', 'gx', 'gy', 'gz')), parts along dimension 1, may hold values 0 or 1
Outputs:
- final_positions: float32 [3, 8, 4096], P(None, None, ('runs', 'gx', 'gy', 'gz')), parts along dimension 2
- final_velocities: float32 [3, 8, 4096], P(None, None, ('runs', 'gx', 'gy', 'gz')), parts along dimension 2
- energies: float32 [6, 2], P('runs'), parts along dimension 0
The draws below stay inside these ranges and needn't reach their ends.
There are 2 independent parts, one for each index of `runs`. The reference program is written for one: setup_inputs(seed, part) draws one part's arguments, and reference() takes and returns one part's arrays. A program takes and returns all parts, laid end to end along the dimension named above; each array names one. Nothing has to cross between parts.
Inputs may be any that keep to these rules, and one draw needn't show every extreme that they name: `send_list`: each domain's 178 entries are its own clusters (0 to 127, counted within the domain), in seven zone blocks of the sizes and order given in the reference program; a cluster may appear in several blocks. `pair_list`: each domain's 1792 slots name clusters of its extended set: 0 to 127 its own, then its received zone blocks in order; padding slots hold 306 in both rows; every cluster appears in a slot with itself; no unordered pair appears twice. `positions`: eight beads of a cluster lie in its cell of side 1, the cells of a domain filling a box of 1 by 8 by 16; neighbouring beads of a cluster are between 0.25 and 0.6 apart.
All inputs are finite; a program needn't handle non-finite values. No bound on the sum of `constraint_flags` on one device may be relied on, other than what follows from the above.
Results may differ from the reference program's by a relative error of at most 0.0003.
Values sent between devices are 32-bit elements; how exact they have to be, the bound alone decides.
No kernel may reach another device: no remote copies, remote signals or barrier semaphores. Data moves between devices by JAX's collectives and lax.ppermute only.
A program may use at most 64 MiB of HBM per device.

```python
import jax
import jax.numpy as jnp
import numpy as np
from jax import lax

CX = 1
CY = 8
CZ = 16
ITERS = 3
NORDER = 4
NITER = 1
CL = 128
HC = 178
NP = 1792
DOMAINS = 16
NCL = 2048
BEADS = 16384
N_GX = 4
N_GY = 2
N_GZ = 2


zone_list = ((1, 0, 0), (0, 1, 0), (0, 0, 1), (1, 1, 0), (1, 0, 1), (0, 1, 1), (1, 1, 1))


def cluster_layout(key):
    layout_key = jax.random.fold_in(key, 101)
    scores = jax.random.randint(layout_key, (DOMAINS, CL), 0, 16384) * CL + jnp.arange(CL, dtype=jnp.int32)[None]
    cell_of_slot = jnp.argsort(scores, axis=1).astype(jnp.int32)
    slot_of_cell = jnp.argsort(cell_of_slot, axis=1).astype(jnp.int32)
    return (cell_of_slot, slot_of_cell)


def zone_cells(direction):
    cell_list = []
    for coord_x in [0] if direction[0] else range(CX):
        for coord_y in [0] if direction[1] else range(CY):
            for coord_z in [0] if direction[2] else range(CZ):
                cell_list.append((coord_x, coord_y, coord_z))
    return cell_list


def send_cells():
    linear = []
    for direction in zone_list:
        for cell in zone_cells(direction):
            linear.append((cell[0] * CY + cell[1]) * CZ + cell[2])
    return np.array(linear, np.int32)


def candidate_pairs():
    home_table = np.full((CX + 1, CY + 1, CZ + 1), -1, np.int32)
    halo_table = np.full((CX + 1, CY + 1, CZ + 1), -1, np.int32)
    for coord_x in range(CX):
        for coord_y in range(CY):
            for coord_z in range(CZ):
                home_table[coord_x, coord_y, coord_z] = (coord_x * CY + coord_y) * CZ + coord_z
    counter = CX * CY * CZ
    for direction in zone_list:
        for cell in zone_cells(direction):
            halo_table[cell[0] + direction[0] * CX, cell[1] + direction[1] * CY, cell[2] + direction[2] * CZ] = counter
            counter += 1
    dim_options = ((0, 0), (0, 1), (1, 0))
    patterns = []
    for first_dim in dim_options:
        for second_dim in dim_options:
            for third_dim in dim_options:
                pattern = (first_dim, second_dim, third_dim)
                leading = [entry for entry in pattern if entry != (0, 0)]
                if not leading or leading[0] == (0, 1):
                    patterns.append(pattern)
    first_home, first_halo, second_home, second_halo = ([], [], [], [])
    for coord_x in range(CX):
        for coord_y in range(CY):
            for coord_z in range(CZ):
                for pattern in patterns:
                    first_cell = (coord_x + pattern[0][0], coord_y + pattern[1][0], coord_z + pattern[2][0])
                    second_cell = (coord_x + pattern[0][1], coord_y + pattern[1][1], coord_z + pattern[2][1])
                    first_home.append(home_table[first_cell])
                    first_halo.append(halo_table[first_cell])
                    second_home.append(home_table[second_cell])
                    second_halo.append(halo_table[second_cell])
    return (np.array(first_home, np.int32), np.array(first_halo, np.int32), np.array(second_home, np.int32), np.array(second_halo, np.int32))


def draw_positions(key, part):
    cell_of_slot, slot_of_cell = cluster_layout(key)
    cell_x = cell_of_slot // (CY * CZ)
    cell_y = cell_of_slot // CZ % CY
    cell_z = cell_of_slot % CZ
    cell_coords = jnp.stack([cell_x, cell_y, cell_z]).astype(jnp.float32)
    beads = jnp.arange(8, dtype=jnp.float32)
    parity = (jnp.arange(8, dtype=jnp.int32) % 2).astype(jnp.float32)
    offsets = jnp.stack([0.115 + 0.11 * beads, 0.3 + 0.4 * parity, 0.115 + 0.11 * beads])
    spread = 0.03
    noise = jax.random.uniform(jax.random.fold_in(key, 202), (3, 8, DOMAINS, CL), jnp.float32, -spread, spread)
    result = cell_coords[:, None] + offsets[:, :, None, None] + noise
    return result.reshape(3, 8, DOMAINS * CL)


def draw_send_list(key, part):
    cell_of_slot, slot_of_cell = cluster_layout(key)
    return slot_of_cell[:, jnp.asarray(send_cells())].reshape(DOMAINS * HC).astype(jnp.int32)


def draw_pair_list(key, part):
    cell_of_slot, slot_of_cell = cluster_layout(key)
    first_home, first_halo, second_home, second_halo = candidate_pairs()
    padding = CL + HC

    def resolve(home_ids, halo_ids):
        from_home = slot_of_cell[:, jnp.asarray(np.maximum(home_ids, 0))]
        return jnp.where(jnp.asarray(home_ids >= 0)[None], from_home, jnp.asarray(halo_ids)[None])
    first_ids = resolve(first_home, first_halo)
    second_ids = resolve(second_home, second_halo)
    self_mask = jnp.asarray((first_home == second_home) & (first_halo == second_halo))[None]
    keep = (jax.random.randint(jax.random.fold_in(key, 303), (DOMAINS, NP), 0, 8) != 0) | self_mask
    first_ids = jnp.where(keep, first_ids, padding)
    second_ids = jnp.where(keep, second_ids, padding)
    order_scores = jax.random.randint(jax.random.fold_in(key, 404), (DOMAINS, NP), 0, 4096) * NP + jnp.arange(NP, dtype=jnp.int32)[None]
    shuffle = jnp.argsort(order_scores, axis=1)
    first_ids = jnp.take_along_axis(first_ids, shuffle, axis=1)
    second_ids = jnp.take_along_axis(second_ids, shuffle, axis=1)
    return jnp.stack([first_ids.reshape(-1), second_ids.reshape(-1)]).astype(jnp.int32)


def with_ends(values, key, smallest, high):
    place = [jax.random.randint(jax.random.fold_in(key, axis), (), 0, length) for axis, length in enumerate(values.shape)]
    longest = values.shape.index(max(values.shape))
    next_to = place[:longest] + [(place[longest] + 1) % values.shape[longest]] + place[longest + 1:]
    return values.at[tuple(place)].set(smallest).at[tuple(next_to)].set(high)


def level_of(stream_key, dims, cuts, least, top_value):
    def one(position, parts):
        heights = jax.random.uniform(jax.random.fold_in(jax.random.fold_in(stream_key, 6), position), (parts,), jnp.float32, least / len(cuts), top_value / len(cuts))
        return jnp.repeat(jnp.exp(heights), dims[position] // parts).reshape((-1,) + (1,) * (len(dims) - position - 1))

    factor_of = one(*cuts[0])
    for cut in cuts[1:]:
        factor_of = factor_of * one(*cut)
    return factor_of


def normal_values(stream_key, dims, scale, limit, shards=(), held_as=jnp.bfloat16):
    drawn = jax.random.normal(stream_key, dims, jnp.float32) * scale
    if len(shards) > 0:
        drawn = level_of(stream_key, dims, shards, -0.22, 0.18) * drawn
    return jnp.clip(drawn, min=-limit, max=limit).astype(held_as)


def setup_inputs(seed: int = 0, part: int = 0) -> dict:
    keys = jax.random.split(jax.random.key(seed), 6)
    own_keys = jax.random.split(jax.random.fold_in(keys[5], part), 6)
    positions = draw_positions(jax.random.fold_in(jax.random.fold_in(keys[5], part), 71), part)
    velocities = normal_values(own_keys[1], (3, 8, NCL), 1.0, 5.0, ((2, 16),), jnp.float32)
    send_list = draw_send_list(jax.random.fold_in(jax.random.fold_in(keys[5], part), 71), part)
    pair_list = draw_pair_list(jax.random.fold_in(jax.random.fold_in(keys[5], part), 71), part)
    constraint_flags = with_ends((jax.random.randint(own_keys[4], (7, NCL), 0, 4) < 3).astype(jnp.int32), jax.random.fold_in(own_keys[4], 1), 0, 1)
    return dict(positions=positions, velocities=velocities, send_list=send_list, pair_list=pair_list, constraint_flags=constraint_flags)


time_step = 0.02
strength = 2.0
root_half = 0.7071067811865476
zone_list = ((1, 0, 0), (0, 1, 0), (0, 0, 1), (1, 1, 0), (1, 0, 1), (0, 1, 1), (1, 1, 1))

def zone_sizes():
    return tuple(((CX if direction[0] == 0 else 1) * (CY if direction[1] == 0 else 1) * (CZ if direction[2] == 0 else 1) for direction in zone_list))

def zone_starts():
    block_sizes = zone_sizes()
    return tuple((sum(block_sizes[:number]) for number in range(7)))

def pair_kernel(extended, first_ids, second_ids):
    dummy_index = extended.shape[2] - 1
    first_coords = jnp.take(extended, first_ids, axis=2)
    second_coords = jnp.take(extended, second_ids, axis=2)
    separation = first_coords[:, :, None, :] - second_coords[:, None, :, :]
    scaled = lax.optimization_barrier(jnp.sum(separation * separation, axis=0))
    intersect = jnp.maximum(1.0 - scaled, 0.0)
    bead_row = lax.broadcasted_iota(jnp.int32, (8, 8, 1), 0)
    bead_column = lax.broadcasted_iota(jnp.int32, (8, 8, 1), 1)
    self_pair = (first_ids == second_ids)[None, None, :]
    usable = (first_ids < dummy_index)[None, None, :]
    weight = (jnp.where(self_pair, bead_row < bead_column, True) & usable).astype(jnp.float32)
    energy = strength * jnp.sum(weight * intersect * intersect * intersect)
    magnitude = 6.0 * strength * weight * intersect * intersect
    pushing = magnitude[None] * separation
    return (lax.optimization_barrier(jnp.sum(pushing, axis=2)), -lax.optimization_barrier(jnp.sum(pushing, axis=1)), energy)

def domain_forces(extended, pair_ids):
    first_blocks = pair_ids[0].reshape(28, -1)
    second_blocks = pair_ids[1].reshape(28, -1)

    def accumulate(state, blocks):
        forces, energy = state
        on_first, on_second, block_energy = pair_kernel(extended, blocks[0], blocks[1])
        forces = forces.at[:, :, blocks[0]].add(on_first)
        forces = forces.at[:, :, blocks[1]].add(on_second)
        return ((forces, energy + block_energy), None)
    initial = (jnp.zeros(extended.shape, jnp.float32), jnp.zeros((), jnp.float32))
    result = lax.scan(accumulate, initial, (first_blocks, second_blocks))
    return result[0]

def total_forces(coords, send_list, pair_list):
    grid_shape = (N_GX, N_GY, N_GZ)
    domain_count = N_GX * N_GY * N_GZ
    home_coords = coords.reshape((3, 8) + grid_shape + (CL,))
    send_grid = send_list.reshape(grid_shape + (HC,))
    block_sizes = zone_sizes()
    starts = zone_starts()
    pieces = []
    for number in range(7):
        direction = zone_list[number]
        backward = tuple((-component for component in direction))
        source = jnp.roll(home_coords, backward, axis=(2, 3, 4))
        chosen = jnp.roll(send_grid, backward, axis=(0, 1, 2))[..., starts[number]:starts[number] + block_sizes[number]]
        chosen = jnp.broadcast_to(chosen[None, None], (3, 8) + grid_shape + (block_sizes[number],))
        gathered = jnp.take_along_axis(source, chosen, axis=5)
        offset = jnp.array([direction[0] * CX, direction[1] * CY, direction[2] * CZ], jnp.float32)
        pieces.append(gathered + offset[:, None, None, None, None, None])
    dummy_cluster = jnp.zeros((3, 8) + grid_shape + (1,), jnp.float32)
    extended = jnp.concatenate([home_coords] + pieces + [dummy_cluster], axis=5)
    extended = jnp.moveaxis(extended.reshape(3, 8, domain_count, CL + HC + 1), 2, 0)
    domain_pairs = jnp.moveaxis(pair_list.reshape(2, domain_count, 14 * CL), 1, 0)
    forces, energies = lax.map(lambda pair_data: domain_forces(pair_data[0], pair_data[1]), (extended, domain_pairs))
    forces = jnp.moveaxis(forces, 0, 2)
    flat_home = forces[:, :, :, :CL].reshape(3, 8, domain_count * CL)
    halo_forces = forces[:, :, :, CL:CL + HC].reshape((3, 8) + grid_shape + (HC,))
    domain_base = (jnp.arange(domain_count, dtype=jnp.int32) * CL).reshape(grid_shape + (1,))
    for number in range(7):
        direction = zone_list[number]
        zone_forces = halo_forces[..., starts[number]:starts[number] + block_sizes[number]]
        zone_forces = jnp.roll(zone_forces, direction, axis=(2, 3, 4))
        targets = (send_grid[..., starts[number]:starts[number] + block_sizes[number]] + domain_base).reshape(-1)
        flat_home = flat_home.at[:, :, targets].add(zone_forces.reshape(3, 8, -1))
    return (flat_home, jnp.sum(energies))

def link_vectors(coords):
    return coords[:, :-1, :] - coords[:, 1:, :]

def link_lengths(coords):
    vectors = link_vectors(coords)
    return jnp.sqrt(lax.optimization_barrier(jnp.sum(vectors * vectors, axis=0)))

def expand(coupling, source):
    coupling_down = jnp.pad(coupling, ((1, 0), (0, 0)))
    coupling_up = jnp.pad(coupling, ((0, 1), (0, 0)))
    series = source
    result = source
    for expansion in range(NORDER):
        series = coupling_down * jnp.pad(series, ((1, 0), (0, 0)))[:-1] + coupling_up * jnp.pad(series, ((0, 1), (0, 0)))[1:]
        result = result + series
    return result

def apply_links(coords, directions, solution):
    shifts = directions * (root_half * solution)[None]
    return coords - jnp.pad(shifts, ((0, 0), (0, 1), (0, 0))) + jnp.pad(shifts, ((0, 0), (1, 0), (0, 0)))

def constrain(previous, updated, rest_length, link_flags):
    old_vectors = link_vectors(previous)
    directions = old_vectors / jnp.maximum(jnp.sqrt(lax.optimization_barrier(jnp.sum(old_vectors * old_vectors, axis=0))), 0.2)[None]
    coupling = 0.5 * lax.optimization_barrier(jnp.sum(directions[:, :-1] * directions[:, 1:], axis=0)) * link_flags[:-1] * link_flags[1:]
    projected = lax.optimization_barrier(jnp.sum(directions * link_vectors(updated), axis=0))
    solution = expand(coupling, link_flags * root_half * (projected - rest_length))
    updated = apply_links(updated, directions, solution)
    for correction in range(NITER):
        vectors = link_vectors(updated)
        squared = lax.optimization_barrier(jnp.sum(vectors * vectors, axis=0))
        target = jnp.sqrt(jnp.maximum(2.0 * rest_length * rest_length - squared, 0.25 * rest_length * rest_length))
        solution = expand(coupling, link_flags * root_half * (rest_length - target))
        updated = apply_links(updated, directions, solution)
    return updated

def reference(positions, velocities, send_list, pair_list, constraint_flags):
    link_flags = constraint_flags.astype(jnp.float32)
    rest_length = link_lengths(positions)
    forces, potential = total_forces(positions, send_list, pair_list)
    energy_rows = []
    for iteration in range(ITERS):
        half_speed = velocities + 0.5 * time_step * forces
        updated = constrain(positions, positions + time_step * half_speed, rest_length, link_flags)
        half_speed = (updated - positions) / time_step
        forces, potential = total_forces(updated, send_list, pair_list)
        velocities = half_speed + 0.5 * time_step * forces
        positions = updated
        kinetic = 0.5 * jnp.sum(velocities * velocities)
        energy_rows.append(jnp.stack([potential, kinetic]))
    energies = jnp.stack(energy_rows) / BEADS
    return (positions, velocities, energies)
```

```python
import jax
import jax.numpy as jnp
import numpy as np
from jax import lax
from jax.sharding import PartitionSpec as P

CX = 1
CY = 8
CZ = 16
ITERS = 3
NORDER = 4


time_step = 0.02
strength = 2.0
root_half = 0.7071067811865476
zone_list = ((1, 0, 0), (0, 1, 0), (0, 0, 1), (1, 1, 0), (1, 0, 1), (0, 1, 1), (1, 1, 1))


def from_behind(value, axis, by):
    count = lax.axis_size(axis)
    return lax.ppermute(value, axis, [(i, (i + by) % count) for i in range(count)])


def zone_sizes():
    return tuple(
        (
            (CX if direction[0] == 0 else 1)
            * (CY if direction[1] == 0 else 1)
            * (CZ if direction[2] == 0 else 1)
            for direction in zone_list
        )
    )


def split_blocks(packed, block_sizes):
    pieces = []
    position = 0
    for length in block_sizes:
        pieces.append(packed[:, :, position : position + length])
        position += length
    return pieces


def shell_offsets():
    block_sizes = zone_sizes()
    columns = []
    for number in range(7):
        direction = zone_list[number]
        column = np.array(
            [[direction[0] * CX], [direction[1] * CY], [direction[2] * CZ]], np.float32
        )
        columns.append(np.tile(column, (1, block_sizes[number])))
    return jnp.asarray(np.concatenate(columns, axis=1))[:, None, :]


def share_coords(coords, send_table):
    sizes_all = zone_sizes()
    chosen = jnp.dot(
        coords.reshape(24, -1), send_table, precision=lax.Precision.HIGHEST
    ).reshape(3, 8, -1)
    outgoing = split_blocks(chosen, sizes_all)
    along_y = from_behind(
        jnp.concatenate([outgoing[1], outgoing[3], outgoing[5], outgoing[6]], axis=2), "gy", -1
    )
    got_y = split_blocks(along_y, [sizes_all[1], sizes_all[3], sizes_all[5], sizes_all[6]])
    along_x = from_behind(
        jnp.concatenate([outgoing[0], outgoing[4], got_y[1], got_y[3]], axis=2), "gx", -1
    )
    got_x = split_blocks(along_x, [sizes_all[0], sizes_all[4], sizes_all[3], sizes_all[6]])
    along_z = from_behind(
        jnp.concatenate([outgoing[2], got_x[1], got_y[2], got_x[3]], axis=2), "gz", -1
    )
    got_z = split_blocks(along_z, [sizes_all[2], sizes_all[4], sizes_all[5], sizes_all[6]])
    received = [got_x[0], got_y[0], got_z[0], got_x[2], got_z[1], got_z[2], got_z[3]]
    return jnp.concatenate(received, axis=2) + shell_offsets()


def return_forces(halo_forces):
    sizes_all = zone_sizes()
    outgoing = split_blocks(halo_forces, sizes_all)
    along_z = from_behind(
        jnp.concatenate([outgoing[2], outgoing[4], outgoing[5], outgoing[6]], axis=2), "gz", 1
    )
    got_z = split_blocks(along_z, [sizes_all[2], sizes_all[4], sizes_all[5], sizes_all[6]])
    along_x = from_behind(
        jnp.concatenate([outgoing[0], outgoing[3], got_z[1], got_z[3]], axis=2), "gx", 1
    )
    got_x = split_blocks(along_x, [sizes_all[0], sizes_all[3], sizes_all[4], sizes_all[6]])
    settled = [got_x[0], got_z[0], got_x[2]]
    pending = [got_x[1], got_z[2], got_x[3]]
    along_y = from_behind(
        jnp.concatenate([outgoing[1], pending[0], pending[1], pending[2]], axis=2), "gy", 1
    )
    got_y = split_blocks(along_y, [sizes_all[1], sizes_all[3], sizes_all[5], sizes_all[6]])
    return jnp.concatenate(
        [settled[0], got_y[0], settled[1], got_y[1], settled[2], got_y[2], got_y[3]], axis=2
    )


def pair_tables(pair_list, extended_count):
    rows = lax.broadcasted_iota(jnp.int32, (extended_count, pair_list.shape[1]), 0)
    first_table = (rows == pair_list[0][None, :]).astype(jnp.float32)
    second_table = (rows == pair_list[1][None, :]).astype(jnp.float32)
    return (first_table, second_table)


def domain_forces(extended, pair_list, tables):
    extended_count = extended.shape[2]
    slot_count = pair_list.shape[1]
    first_ids = pair_list[0]
    second_ids = pair_list[1]
    flat = extended.reshape(24, extended_count)
    first_coords = jnp.dot(flat, tables[0], precision=lax.Precision.HIGHEST).reshape(
        3, 8, slot_count
    )
    second_coords = jnp.dot(flat, tables[1], precision=lax.Precision.HIGHEST).reshape(
        3, 8, slot_count
    )
    separation = first_coords[:, :, None, :] - second_coords[:, None, :, :]
    scaled = jnp.sum(separation * separation, axis=0)
    intersect = jnp.maximum(1.0 - scaled, 0.0)
    bead_row = lax.broadcasted_iota(jnp.int32, (8, 8, 1), 0)
    bead_column = lax.broadcasted_iota(jnp.int32, (8, 8, 1), 1)
    self_pair = (first_ids == second_ids)[None, None, :]
    usable = (first_ids < extended_count - 1)[None, None, :]
    weight = (jnp.where(self_pair, bead_row < bead_column, True) & usable).astype(jnp.float32)
    energy = strength * jnp.sum(weight * intersect * intersect * intersect)
    magnitude = 6.0 * strength * weight * intersect * intersect
    pushing = magnitude[None] * separation
    on_first = jnp.sum(pushing, axis=2).reshape(24, slot_count)
    on_second = (-jnp.sum(pushing, axis=1)).reshape(24, slot_count)
    contract = (((1,), (1,)), ((), ()))
    forces = lax.dot_general(on_first, tables[0], contract, precision=lax.Precision.HIGHEST)
    forces = forces + lax.dot_general(
        on_second, tables[1], contract, precision=lax.Precision.HIGHEST
    )
    return (forces.reshape(3, 8, extended_count), energy)


def local_forces(coords, send_table, pair_list, tables):
    halo_coords = share_coords(coords, send_table)
    dummy_cluster = jnp.zeros((3, 8, 1), jnp.float32)
    extended = jnp.concatenate([coords, halo_coords, dummy_cluster], axis=2)
    forces, energy = domain_forces(extended, pair_list, tables)
    cluster_count = coords.shape[2]
    returned = return_forces(forces[:, :, cluster_count : cluster_count + send_table.shape[1]])
    contract = (((1,), (1,)), ((), ()))
    added = lax.dot_general(
        returned.reshape(24, -1), send_table, contract, precision=lax.Precision.HIGHEST
    )
    home_forces = forces[:, :, :cluster_count] + added.reshape(3, 8, -1)
    return (home_forces, energy)


def link_vectors(coords):
    return coords[:, :-1, :] - coords[:, 1:, :]


def link_lengths(coords):
    vectors = link_vectors(coords)
    return jnp.sqrt(jnp.sum(vectors * vectors, axis=0))


def expand(coupling, source):
    coupling_down = jnp.pad(coupling, ((1, 0), (0, 0)))
    coupling_up = jnp.pad(coupling, ((0, 1), (0, 0)))
    series = source
    result = source
    for expansion in range(NORDER):
        series = (
            coupling_down * jnp.pad(series, ((1, 0), (0, 0)))[:-1]
            + coupling_up * jnp.pad(series, ((0, 1), (0, 0)))[1:]
        )
        result = result + series
    return result


def apply_links(coords, directions, solution):
    shifts = directions * (root_half * solution)[None]
    return (
        coords
        - jnp.pad(shifts, ((0, 0), (0, 1), (0, 0)))
        + jnp.pad(shifts, ((0, 0), (1, 0), (0, 0)))
    )


def constrain(previous, updated, rest_length, link_flags):
    old_vectors = link_vectors(previous)
    directions = (
        old_vectors / jnp.maximum(jnp.sqrt(jnp.sum(old_vectors * old_vectors, axis=0)), 0.2)[None]
    )
    coupling = (
        0.5
        * jnp.sum(directions[:, :-1] * directions[:, 1:], axis=0)
        * link_flags[:-1]
        * link_flags[1:]
    )
    projected = jnp.sum(directions * link_vectors(updated), axis=0)
    solution = expand(coupling, link_flags * root_half * (projected - rest_length))
    updated = apply_links(updated, directions, solution)
    vectors = link_vectors(updated)
    squared = jnp.sum(vectors * vectors, axis=0)
    target = jnp.sqrt(
        jnp.maximum(2.0 * rest_length * rest_length - squared, 0.25 * rest_length * rest_length)
    )
    solution = expand(coupling, link_flags * root_half * (rest_length - target))
    updated = apply_links(updated, directions, solution)
    return updated


def total_over(value, axis):
    count = lax.axis_size(axis)
    if count > 4:
        return lax.psum(value, axis)
    total = value
    for by in range(1, count):
        total = total + from_behind(value, axis, by)
    return total


def on_device(positions, velocities, send_list, pair_list, constraint_flags):
    link_flags = constraint_flags.astype(jnp.float32)
    rest_length = link_lengths(positions)
    bead_total = 8 * positions.shape[2] * lax.axis_size(("gx", "gy", "gz"))
    tables = pair_tables(pair_list, positions.shape[2] + send_list.shape[0] + 1)
    owned = lax.broadcasted_iota(jnp.int32, (positions.shape[2], send_list.shape[0]), 0)
    send_table = (owned == send_list[None, :]).astype(jnp.float32)
    forces, potential = local_forces(positions, send_table, pair_list, tables)
    energy_rows = []
    for iteration in range(ITERS):
        half_speed = velocities + 0.5 * time_step * forces
        updated = constrain(positions, positions + time_step * half_speed, rest_length, link_flags)
        half_speed = (updated - positions) / time_step
        forces, potential = local_forces(updated, send_table, pair_list, tables)
        velocities = half_speed + 0.5 * time_step * forces
        positions = updated
        kinetic = 0.5 * jnp.sum(velocities * velocities)
        energy_rows.append(jnp.stack([potential, kinetic]))
    energies = jnp.stack(energy_rows)
    for axis in ("gz", "gy", "gx"):
        energies = total_over(energies, axis)
    return (positions, velocities, energies / bead_total)


def solution(mesh):
    return jax.shard_map(
        on_device,
        mesh=mesh,
        in_specs=(
            P(None, None, ("runs", "gx", "gy", "gz")),
            P(None, None, ("runs", "gx", "gy", "gz")),
            P(("runs", "gx", "gy", "gz")),
            P(None, ("runs", "gx", "gy", "gz")),
            P(None, ("runs", "gx", "gy", "gz")),
        ),
        out_specs=(
            P(None, None, ("runs", "gx", "gy", "gz")),
            P(None, None, ("runs", "gx", "gy", "gz")),
            P("runs", None),
        ),
        check_vma=False,
    )
```

```python
import functools

import jax
import jax.numpy as jnp
import numpy as np
from jax import lax
from jax.experimental import pallas as pl
from jax.experimental.pallas import tpu as pltpu
from jax.sharding import PartitionSpec as P

CX = 1
CY = 8
CZ = 16
ITERS = 3
NORDER = 4


time_step = 0.02
strength = 2.0
root_half = 0.7071067811865476
zone_list = ((1, 0, 0), (0, 1, 0), (0, 0, 1), (1, 1, 0), (1, 0, 1), (0, 1, 1), (1, 1, 1))


def from_behind(value, axis, by):
    count = lax.axis_size(axis)
    return lax.ppermute(value, axis, [(i, (i + by) % count) for i in range(count)])


def zone_sizes():
    return tuple(
        (
            (CX if direction[0] == 0 else 1)
            * (CY if direction[1] == 0 else 1)
            * (CZ if direction[2] == 0 else 1)
            for direction in zone_list
        )
    )


def split_blocks(packed, block_sizes):
    pieces = []
    position = 0
    for length in block_sizes:
        pieces.append(packed[:, :, position : position + length])
        position += length
    return pieces


def shell_offsets():
    block_sizes = zone_sizes()
    columns = []
    for number in range(7):
        direction = zone_list[number]
        column = np.array(
            [[direction[0] * CX], [direction[1] * CY], [direction[2] * CZ]], np.float32
        )
        columns.append(np.tile(column, (1, block_sizes[number])))
    return jnp.asarray(np.concatenate(columns, axis=1))[:, None, :]


def share_coords(coords, send_table):
    sizes_all = zone_sizes()
    chosen = jnp.dot(
        coords.reshape(24, -1), send_table, precision=lax.Precision.HIGHEST
    ).reshape(3, 8, -1)
    outgoing = split_blocks(chosen, sizes_all)
    along_y = from_behind(
        jnp.concatenate([outgoing[1], outgoing[3], outgoing[5], outgoing[6]], axis=2), "gy", -1
    )
    got_y = split_blocks(along_y, [sizes_all[1], sizes_all[3], sizes_all[5], sizes_all[6]])
    along_x = from_behind(
        jnp.concatenate([outgoing[0], outgoing[4], got_y[1], got_y[3]], axis=2), "gx", -1
    )
    got_x = split_blocks(along_x, [sizes_all[0], sizes_all[4], sizes_all[3], sizes_all[6]])
    along_z = from_behind(
        jnp.concatenate([outgoing[2], got_x[1], got_y[2], got_x[3]], axis=2), "gz", -1
    )
    got_z = split_blocks(along_z, [sizes_all[2], sizes_all[4], sizes_all[5], sizes_all[6]])
    received = [got_x[0], got_y[0], got_z[0], got_x[2], got_z[1], got_z[2], got_z[3]]
    return jnp.concatenate(received, axis=2) + shell_offsets()


def return_forces(halo_forces):
    sizes_all = zone_sizes()
    outgoing = split_blocks(halo_forces, sizes_all)
    along_z = from_behind(
        jnp.concatenate([outgoing[2], outgoing[4], outgoing[5], outgoing[6]], axis=2), "gz", 1
    )
    got_z = split_blocks(along_z, [sizes_all[2], sizes_all[4], sizes_all[5], sizes_all[6]])
    along_x = from_behind(
        jnp.concatenate([outgoing[0], outgoing[3], got_z[1], got_z[3]], axis=2), "gx", 1
    )
    got_x = split_blocks(along_x, [sizes_all[0], sizes_all[3], sizes_all[4], sizes_all[6]])
    settled = [got_x[0], got_z[0], got_x[2]]
    pending = [got_x[1], got_z[2], got_x[3]]
    along_y = from_behind(
        jnp.concatenate([outgoing[1], pending[0], pending[1], pending[2]], axis=2), "gy", 1
    )
    got_y = split_blocks(along_y, [sizes_all[1], sizes_all[3], sizes_all[5], sizes_all[6]])
    return jnp.concatenate(
        [settled[0], got_y[0], settled[1], got_y[1], settled[2], got_y[2], got_y[3]], axis=2
    )


def pair_tables(pair_list, extended_count):
    rows = lax.broadcasted_iota(jnp.int32, (extended_count, pair_list.shape[1]), 0)
    first_table = (rows == pair_list[0][None, :]).astype(jnp.float32)
    second_table = (rows == pair_list[1][None, :]).astype(jnp.float32)
    return (first_table, second_table)


def domain_forces(extended, pair_list, tables):
    extended_count = extended.shape[2]
    slot_count = pair_list.shape[1]
    first_ids = pair_list[0]
    second_ids = pair_list[1]
    flat = extended.reshape(24, extended_count)
    first_coords = jnp.dot(flat, tables[0], precision=lax.Precision.HIGHEST).reshape(
        3, 8, slot_count
    )
    second_coords = jnp.dot(flat, tables[1], precision=lax.Precision.HIGHEST).reshape(
        3, 8, slot_count
    )
    separation = first_coords[:, :, None, :] - second_coords[:, None, :, :]
    scaled = jnp.sum(separation * separation, axis=0)
    intersect = jnp.maximum(1.0 - scaled, 0.0)
    bead_row = lax.broadcasted_iota(jnp.int32, (8, 8, 1), 0)
    bead_column = lax.broadcasted_iota(jnp.int32, (8, 8, 1), 1)
    self_pair = (first_ids == second_ids)[None, None, :]
    usable = (first_ids < extended_count - 1)[None, None, :]
    weight = (jnp.where(self_pair, bead_row < bead_column, True) & usable).astype(jnp.float32)
    energy = strength * jnp.sum(weight * intersect * intersect * intersect)
    magnitude = 6.0 * strength * weight * intersect * intersect
    pushing = magnitude[None] * separation
    on_first = jnp.sum(pushing, axis=2).reshape(24, slot_count)
    on_second = (-jnp.sum(pushing, axis=1)).reshape(24, slot_count)
    contract = (((1,), (1,)), ((), ()))
    forces = lax.dot_general(on_first, tables[0], contract, precision=lax.Precision.HIGHEST)
    forces = forces + lax.dot_general(
        on_second, tables[1], contract, precision=lax.Precision.HIGHEST
    )
    return (forces.reshape(3, 8, extended_count), energy)


def local_forces(coords, send_table, pair_list, tables):
    halo_coords = share_coords(coords, send_table)
    dummy_cluster = jnp.zeros((3, 8, 1), jnp.float32)
    extended = jnp.concatenate([coords, halo_coords, dummy_cluster], axis=2)
    forces, energy = domain_forces(extended, pair_list, tables)
    cluster_count = coords.shape[2]
    returned = return_forces(forces[:, :, cluster_count : cluster_count + send_table.shape[1]])
    contract = (((1,), (1,)), ((), ()))
    added = lax.dot_general(
        returned.reshape(24, -1), send_table, contract, precision=lax.Precision.HIGHEST
    )
    home_forces = forces[:, :, :cluster_count] + added.reshape(3, 8, -1)
    return (home_forces, energy)


def link_vectors(coords):
    return coords[:, :-1, :] - coords[:, 1:, :]


def link_lengths(coords):
    vectors = link_vectors(coords)
    return jnp.sqrt(jnp.sum(vectors * vectors, axis=0))


def expand(coupling, source):
    coupling_down = jnp.pad(coupling, ((1, 0), (0, 0)))
    coupling_up = jnp.pad(coupling, ((0, 1), (0, 0)))
    series = source
    result = source
    for expansion in range(NORDER):
        series = (
            coupling_down * jnp.pad(series, ((1, 0), (0, 0)))[:-1]
            + coupling_up * jnp.pad(series, ((0, 1), (0, 0)))[1:]
        )
        result = result + series
    return result


def apply_links(coords, directions, solution):
    shifts = directions * (root_half * solution)[None]
    return (
        coords
        - jnp.pad(shifts, ((0, 0), (0, 1), (0, 0)))
        + jnp.pad(shifts, ((0, 0), (1, 0), (0, 0)))
    )


def constrain(previous, updated, rest_length, link_flags):
    old_vectors = link_vectors(previous)
    directions = (
        old_vectors / jnp.maximum(jnp.sqrt(jnp.sum(old_vectors * old_vectors, axis=0)), 0.2)[None]
    )
    coupling = (
        0.5
        * jnp.sum(directions[:, :-1] * directions[:, 1:], axis=0)
        * link_flags[:-1]
        * link_flags[1:]
    )
    projected = jnp.sum(directions * link_vectors(updated), axis=0)
    solution = expand(coupling, link_flags * root_half * (projected - rest_length))
    updated = apply_links(updated, directions, solution)
    vectors = link_vectors(updated)
    squared = jnp.sum(vectors * vectors, axis=0)
    target = jnp.sqrt(
        jnp.maximum(2.0 * rest_length * rest_length - squared, 0.25 * rest_length * rest_length)
    )
    solution = expand(coupling, link_flags * root_half * (rest_length - target))
    updated = apply_links(updated, directions, solution)
    return updated


def total_over(value, axis):
    count = lax.axis_size(axis)
    if count > 4:
        return lax.psum(value, axis)
    total = value
    for by in range(1, count):
        total = total + from_behind(value, axis, by)
    return total


def on_device(positions, velocities, send_list, pair_list, constraint_flags):
    link_flags = constraint_flags.astype(jnp.float32)
    rest_length = link_lengths(positions)
    bead_total = 8 * positions.shape[2] * lax.axis_size(("gx", "gy", "gz"))
    tables = pair_tables(pair_list, positions.shape[2] + send_list.shape[0] + 1)
    owned = lax.broadcasted_iota(jnp.int32, (positions.shape[2], send_list.shape[0]), 0)
    send_table = (owned == send_list[None, :]).astype(jnp.float32)
    forces, potential = local_forces(positions, send_table, pair_list, tables)
    energy_rows = []
    for iteration in range(ITERS):
        half_speed = velocities + 0.5 * time_step * forces
        updated = constrain(positions, positions + time_step * half_speed, rest_length, link_flags)
        half_speed = (updated - positions) / time_step
        forces, potential = local_forces(updated, send_table, pair_list, tables)
        velocities = half_speed + 0.5 * time_step * forces
        positions = updated
        kinetic = 0.5 * jnp.sum(velocities * velocities)
        energy_rows.append(jnp.stack([potential, kinetic]))
    energies = jnp.stack(energy_rows)
    for axis in ("gz", "gy", "gx"):
        energies = total_over(energies, axis)
    return (positions, velocities, energies / bead_total)


LANES = 128
ROWS = 24
MAX_REPLICATED = 16


def split_rows(value):
    high = value.astype(jnp.bfloat16).astype(jnp.float32)
    return jnp.concatenate([high, value - high], axis=0).astype(jnp.bfloat16)


def joined(value):
    return value[:ROWS] + value[ROWS:]


class Grid:
    def __init__(self, mesh, slot_count, halo_count):
        self.gx, self.gy, self.gz = (mesh.shape[a] for a in ("gx", "gy", "gz"))
        self.domains = self.gx * self.gy * self.gz
        self.lists = self.gx * self.gy
        self.blocks = slot_count // LANES
        self.padded = (self.blocks + 7) // 8 * 8
        self.dummy = LANES + halo_count
        self.slots = 2 * self.blocks * LANES
        sizes = zone_sizes()
        self.zones = []
        start = 0
        for direction, size in zip(zone_list[1:], sizes[1:]):
            self.zones.append((direction, start, start + size))
            start += size

    def domain(self, i, j, direction):
        i = lax.rem(i + direction[0], self.gx) if not isinstance(i, int) else (i + direction[0]) % self.gx
        j = lax.rem(j + direction[1], self.gy) if not isinstance(j, int) else (j + direction[1]) % self.gy
        return (i * self.gy + j) * self.gz + direction[2] % self.gz

    def rows_of(self, i, j, direction):
        row = self.domain(i, j, direction) * 8
        return pl.ds(row if isinstance(row, int) else pl.multiple_of(row, 8), 8)


def lanes_of(shape):
    return lax.broadcasted_iota(jnp.int32, shape, 1)


def take_lanes(source, index):
    return jnp.take_along_axis(source, index, axis=1, mode="promise_in_bounds")


def build_tables(grid, near_ref, far_ref, pair_row, send_row, ids_ref, weight_ref, index_ref, table_ref, zone_ref):
    blocks = grid.blocks
    lane = lanes_of((8, LANES))
    own_code = lanes_of((LANES, LANES)).astype(jnp.float32).astype(jnp.bfloat16)
    first_code = (lanes_of((LANES, LANES)) + LANES).astype(jnp.float32).astype(jnp.bfloat16)
    rest_code = (-1 - lanes_of((LANES, LANES))).astype(jnp.float32).astype(jnp.bfloat16)
    one = jnp.ones((LANES, LANES), jnp.bfloat16)
    zero = jnp.zeros((LANES, LANES), jnp.bfloat16)

    def send_of(number, row):
        source = near_ref if number % grid.gz == 0 else far_ref
        return source[number // grid.gz, pl.ds(send_row + row, 1), :]

    for number in range(grid.lists):
        i, j = number // grid.gy, number % grid.gy
        to_x = send_of(grid.domain(i, j, zone_list[0]), 0)
        rest = jnp.zeros((1, LANES), jnp.float32)
        for direction, start, stop in grid.zones:
            row = send_of(grid.domain(i, j, direction), 1)
            rest = jnp.where((lane[:1] >= start) & (lane[:1] < stop), row, rest)
        both = jnp.concatenate([to_x, rest] + [jnp.zeros((6, LANES), jnp.float32)], axis=0)
        index_ref[number] = both.astype(jnp.int32)

    def one_list(number, carry):
        first = near_ref[number, pl.ds(pair_row, blocks), :]
        second = near_ref[number, pl.ds(pair_row + blocks, blocks), :]
        fill = jnp.full((grid.padded - blocks, LANES), float(grid.dummy), jnp.float32)
        parts = [[first, fill], [second, fill]] if grid.padded > blocks else [[first], [second]]
        first, second = (jnp.concatenate(p, axis=0) for p in parts)
        ids_ref[0, number] = first.astype(jnp.int32)
        ids_ref[1, number] = second.astype(jnp.int32)
        usable = jnp.where(first < float(grid.dummy), 1.0, 0.0)
        weight_ref[number] = jnp.where(first == second, 0.5, 1.0) * usable
        both = index_ref[number].astype(jnp.float32)
        codes = jnp.concatenate([first, second], axis=0)
        codes = jnp.where(codes < 2.0 * LANES, codes, 2.0 * LANES - 1.0 - codes)
        turned = jnp.transpose(jnp.concatenate([codes, both], axis=0))
        for side in range(2):
            for block in range(blocks):
                at = side * grid.padded + block
                column = jnp.broadcast_to(turned[:, at : at + 1], (LANES, LANES)).astype(jnp.bfloat16)
                rows = pl.ds((side * blocks + block) * LANES, LANES)
                for part, code in enumerate((own_code, first_code, rest_code)):
                    table_ref[number, rows, pl.ds(part * LANES, LANES)] = jnp.where(column == code, one, zero)
        at = 2 * grid.padded
        column = jnp.broadcast_to(turned[:, at : at + 1], (LANES, LANES)).astype(jnp.bfloat16)
        zone_ref[number, :, pl.ds(0, LANES)] = jnp.where(column == own_code, one, zero)
        column = jnp.broadcast_to(turned[:, at + 1 : at + 2], (LANES, LANES)).astype(jnp.bfloat16)
        slot = lax.broadcasted_iota(jnp.int32, (LANES, LANES), 0).astype(jnp.float32).astype(jnp.bfloat16)
        for part, (direction, start, stop) in enumerate(grid.zones):
            here = (column == own_code) & (slot >= start) & (slot < stop)
            zone_ref[number, :, pl.ds((part + 1) * LANES, LANES)] = jnp.where(here, one, zero)
        return carry

    lax.fori_loop(0, grid.lists, one_list, 0)


def gather_and_push(grid, number, x_ref, ids_ref, weight_ref, index_ref, ext_ref, push_ref, energy_ref):
    i, j = lax.div(number, grid.gy), lax.rem(number, grid.gy)
    lane = lanes_of((8, LANES))
    cell = (CX, CY, CZ)
    to_x = jnp.broadcast_to(index_ref[number, pl.ds(0, 1), :], (8, LANES))
    rest = jnp.broadcast_to(index_ref[number, pl.ds(1, 1), :], (8, LANES))
    for c in range(3):
        ext_ref[c, 0] = x_ref[c, grid.rows_of(i, j, (0, 0, 0)), :]
        shift = float(zone_list[0][c] * cell[c])
        ext_ref[c, 1] = take_lanes(x_ref[c, grid.rows_of(i, j, zone_list[0]), :], to_x) + shift
        value = jnp.zeros((8, LANES), jnp.float32)
        for direction, start, stop in grid.zones:
            shift = float(direction[c] * cell[c])
            got = take_lanes(x_ref[c, grid.rows_of(i, j, direction), :], rest) + shift
            value = jnp.where((lane >= start) & (lane < stop), got, value)
        ext_ref[c, 2] = value
    for group in range(grid.padded // 8):
        sides = []
        for side in range(2):
            ids = ids_ref[side, number, pl.ds(8 * group, 8), :]
            low = ids & (LANES - 1)
            in_own = ids < LANES
            in_first = ids < 2 * LANES
            coords = []
            for c in range(3):
                line = []
                for bead in range(8):
                    a, b, d = (
                        take_lanes(jnp.broadcast_to(ext_ref[c, part, pl.ds(bead, 1), :], (8, LANES)), low)
                        for part in range(3)
                    )
                    line.append(jnp.where(in_own, a, jnp.where(in_first, b, d)))
                coords.append(line)
            sides.append(coords)
        weight = weight_ref[number, pl.ds(8 * group, 8), :]
        scale = weight * (6.0 * strength)
        energy = None
        on_second = [[None] * 8 for _ in range(3)]
        for k in range(8):
            on_first = [None] * 3
            for l in range(8):
                apart = [sides[0][c][k] - sides[1][c][l] for c in range(3)]
                scaled = apart[0] * apart[0] + apart[1] * apart[1] + apart[2] * apart[2]
                intersect = jnp.maximum(1.0 - scaled, 0.0)
                square = intersect * intersect
                cube = square * intersect
                energy = cube if energy is None else energy + cube
                for c in range(3):
                    pushing = square * apart[c]
                    on_first[c] = pushing if l == 0 else on_first[c] + pushing
                    on_second[c][l] = pushing if k == 0 else on_second[c][l] + pushing
            for c in range(3):
                row = (8 * group) * ROWS + c * 8 + k
                push_ref[pl.ds(row, 8, stride=ROWS), :] = on_first[c] * scale
        for c in range(3):
            for l in range(8):
                row = (grid.padded + 8 * group) * ROWS + c * 8 + l
                push_ref[pl.ds(row, 8, stride=ROWS), :] = -(on_second[c][l] * scale)
        own_beads = jnp.where(weight == 0.5, 8.0, 0.0)
        energy_ref[...] += strength * weight * (energy - own_beads)


def scatter(grid, number, push_ref, table_ref, force_ref, halo_ref):
    pieces = []
    for side in range(2):
        for block in range(grid.blocks):
            pieces.append(push_ref[pl.ds((side * grid.padded + block) * ROWS, ROWS), :])
    pushes = split_rows(jnp.concatenate(pieces, axis=1))
    sums = joined(jnp.dot(pushes, table_ref[number], preferred_element_type=jnp.float32))
    row = pl.multiple_of(number * grid.gz * 8, 8)
    for c in range(3):
        force_ref[pl.ds(c * grid.domains * 8 + row, 8), :] = sums[8 * c : 8 * c + 8, :LANES]
    halo_ref[number] = sums[:, LANES:]


def pair_forces(grid, x_ref, tables, force_ref, scratch):
    ids_ref, weight_ref, index_ref, table_ref, zone_ref = tables
    ext_a, ext_b, push_a, push_b, halo_ref, energy_ref = scratch
    force_ref[...] = jnp.zeros(force_ref.shape, jnp.float32)
    energy_ref[...] = jnp.zeros((8, LANES), jnp.float32)

    def forward(number, ext_ref, push_ref):
        gather_and_push(grid, number, x_ref, ids_ref, weight_ref, index_ref, ext_ref, push_ref, energy_ref)

    def back(number, push_ref):
        scatter(grid, number, push_ref, table_ref, force_ref, halo_ref)

    forward(0, ext_a, push_a)

    def two(m, carry):
        back(2 * m, push_a)
        forward(2 * m + 1, ext_b, push_b)
        back(2 * m + 1, push_b)
        forward(2 * m + 2, ext_a, push_a)
        return carry

    lax.fori_loop(0, grid.lists // 2 - 1, two, 0)
    back(grid.lists - 2, push_a)
    forward(grid.lists - 1, ext_b, push_b)
    back(grid.lists - 1, push_b)
    for number in range(grid.lists):
        i, j = number // grid.gy, number % grid.gy
        halo = halo_ref[number]
        to_x = joined(
            jnp.dot(split_rows(halo[:, :LANES]), zone_ref[number, :, pl.ds(0, LANES)], preferred_element_type=jnp.float32)
        )
        rest = joined(
            jnp.dot(
                split_rows(halo[:, LANES:]),
                zone_ref[number, :, pl.ds(LANES, len(grid.zones) * LANES)],
                preferred_element_type=jnp.float32,
            )
        )
        targets = [(zone_list[0], to_x)]
        for part, (direction, start, stop) in enumerate(grid.zones):
            targets.append((direction, rest[:, part * LANES : (part + 1) * LANES]))
        for direction, value in targets:
            row = grid.domain(i, j, direction) * 8
            for c in range(3):
                force_ref[pl.ds(c * grid.domains * 8 + row, 8), :] += value[8 * c : 8 * c + 8]
    force_ref[pl.ds(3 * grid.domains * 8, 8), :] = energy_ref[...]


def start_kernel(grid, layout, near_ref, far_ref, *refs):
    x_ref, v_ref, rest_ref, flag_ref, ids_ref, weight_ref, index_ref, table_ref, zone_ref, force_ref = refs[:10]
    scratch = refs[10:]
    for number in range(grid.domains):
        source = near_ref if number % grid.gz == 0 else far_ref
        at = number // grid.gz
        rows = pl.ds(number * 8, 8)
        for c in range(3):
            x_ref[c, rows, :] = source[at, pl.ds(layout["positions"] + 8 * c, 8), :]
            v_ref[c, rows, :] = source[at, pl.ds(layout["velocities"] + 8 * c, 8), :]
        flag_ref[rows, :] = source[at, pl.ds(layout["flags"], 8), :]
    rest_ref[...] = link_length([x_ref[c] for c in range(3)])
    build_tables(grid, near_ref, far_ref, layout["pairs"], layout["sends"], ids_ref, weight_ref, index_ref, table_ref, zone_ref)
    pair_forces(grid, x_ref, (ids_ref, weight_ref, index_ref, table_ref, zone_ref), force_ref, scratch)


def up(value):
    return pltpu.roll(value, value.shape[0] - 1, 0)


def down(value):
    return pltpu.roll(value, 1, 0)


def dot3(a, b):
    return a[0] * b[0] + a[1] * b[1] + a[2] * b[2]


def links_of(x):
    return [c - up(c) for c in x]


def link_length(x):
    vectors = links_of(x)
    return jnp.sqrt(dot3(vectors, vectors))


def expand_rows(coupling, before, source):
    series = source
    result = source
    for expansion in range(NORDER):
        series = before * down(series) + coupling * up(series)
        result = result + series
    return result


def apply_rows(x, directions, solution):
    moved = []
    for c in range(3):
        shift = directions[c] * (root_half * solution)
        moved.append(x[c] - shift + down(shift))
    return moved


def constrain_rows(previous, updated, rest, flags):
    old = links_of(previous)
    length = jnp.maximum(jnp.sqrt(dot3(old, old)), 0.2)
    directions = [c / length for c in old]
    coupling = 0.5 * dot3(directions, [up(c) for c in directions]) * flags * up(flags)
    before = down(coupling)
    projected = dot3(directions, links_of(updated))
    solution = expand_rows(coupling, before, flags * (root_half * (projected - rest)))
    updated = apply_rows(updated, directions, solution)
    vectors = links_of(updated)
    squared = dot3(vectors, vectors)
    target = jnp.sqrt(jnp.maximum(2.0 * rest * rest - squared, 0.25 * rest * rest))
    solution = expand_rows(coupling, before, flags * (root_half * (rest - target)))
    return apply_rows(updated, directions, solution)


def total_force(grid, own_ref, got_refs):
    size = grid.domains * 8
    total = []
    for c in range(3):
        pieces = []
        for number in range(grid.domains):
            base, k = number // grid.gz * grid.gz, number % grid.gz
            value = own_ref[pl.ds(c * size + number * 8, 8), :]
            for by, ref in enumerate(got_refs, 1):
                value = value + ref[pl.ds(c * size + (base + (k - by) % grid.gz) * 8, 8), :]
            pieces.append(value)
        total.append(jnp.concatenate(pieces, axis=0))
    return total


def energy_row(grid, own_ref, got_refs, v, row, previous):
    rows = pl.ds(3 * grid.domains * 8, 8)
    potential = own_ref[rows, :]
    for ref in got_refs:
        potential = potential + ref[rows, :]
    kinetic = 0.5 * dot3(v, v)
    lane = lanes_of((8, LANES))
    at = lax.broadcasted_iota(jnp.int32, (8, LANES), 0) == row
    previous = jnp.where(at & (lane == 0), jnp.sum(potential), previous)
    return jnp.where(at & (lane == 1), jnp.sum(kinetic), previous)


def step_kernel(grid, step, x_ref, v_ref, rest_ref, flag_ref, ids_ref, weight_ref, index_ref, table_ref, zone_ref, energies_ref, own_ref, *refs):
    got_refs, refs = refs[: grid.gz - 1], refs[grid.gz - 1 :]
    moved_ref, half_ref, energy_out_ref, force_ref = refs[:4]
    scratch = refs[4:]
    force = total_force(grid, own_ref, got_refs)
    x = [x_ref[c] for c in range(3)]
    v = [v_ref[c] for c in range(3)]
    if step > 0:
        v = [v[c] + (0.5 * time_step) * force[c] for c in range(3)]
        energy_out_ref[...] = energy_row(grid, own_ref, got_refs, v, step - 1, energies_ref[...])
    else:
        energy_out_ref[...] = energies_ref[...]
    half = [v[c] + (0.5 * time_step) * force[c] for c in range(3)]
    moved = constrain_rows(x, [x[c] + time_step * half[c] for c in range(3)], rest_ref[...], flag_ref[...])
    for c in range(3):
        moved_ref[c] = moved[c]
        half_ref[c] = (moved[c] - x[c]) / time_step
    pair_forces(grid, moved_ref, (ids_ref, weight_ref, index_ref, table_ref, zone_ref), force_ref, scratch)


def last_kernel(grid, v_ref, energies_ref, own_ref, *refs):
    got_refs, (speed_ref, energy_out_ref) = refs[: grid.gz - 1], refs[grid.gz - 1 :]
    force = total_force(grid, own_ref, got_refs)
    v = [v_ref[c] + (0.5 * time_step) * force[c] for c in range(3)]
    for c in range(3):
        speed_ref[c] = v[c][:8]
    energy_out_ref[...] = energy_row(grid, own_ref, got_refs, v, ITERS - 1, energies_ref[...])


def from_ahead(value, steps):
    names = [a for a, by in zip(("gx", "gy", "gz"), steps) if by]
    if not names:
        return value
    counts = [lax.axis_size(a) for a in names]
    pairs = []
    for target in np.ndindex(*counts):
        source = [(t + by) % n for t, by, n in zip(target, [s for s in steps if s], counts)]
        pairs.append(tuple(int(np.ravel_multi_index(p, counts)) for p in (source, target)))
    return lax.ppermute(value, tuple(names), pairs)


def replicated(grid, positions, velocities, send_list, pair_list, constraint_flags):
    clusters = positions.shape[2]
    sends = jnp.pad(send_list, (0, -send_list.shape[0] % LANES)).reshape(-1, LANES)
    parts = dict(
        positions=positions.reshape(ROWS, clusters),
        velocities=velocities.reshape(ROWS, clusters),
        flags=jnp.pad(constraint_flags.astype(jnp.float32), ((0, 1), (0, 0))),
        pairs=pair_list.astype(jnp.float32).reshape(-1, LANES),
        sends=sends.astype(jnp.float32),
    )
    layout, row = {}, 0
    for name, value in parts.items():
        layout[name] = row
        row += value.shape[0]
    pack = jnp.concatenate(list(parts.values()) + [jnp.zeros((-row % 8, LANES), jnp.float32)], axis=0)
    near = jnp.stack([from_ahead(pack, (i, j, 0)) for i in range(grid.gx) for j in range(grid.gy)])
    far = from_ahead(near, (0, 0, 1))
    f32, i32, b16 = jnp.float32, jnp.int32, jnp.bfloat16
    n, rows = grid.lists, grid.domains * 8
    cube = jax.ShapeDtypeStruct((3, rows, LANES), f32)
    plane = jax.ShapeDtypeStruct((rows, LANES), f32)
    small = jax.ShapeDtypeStruct((8, LANES), f32)
    forces = jax.ShapeDtypeStruct((3 * rows + 8, LANES), f32)
    table_shapes = [
        jax.ShapeDtypeStruct((2, n, grid.padded, LANES), i32),
        jax.ShapeDtypeStruct((n, grid.padded, LANES), f32),
        jax.ShapeDtypeStruct((n, 8, LANES), i32),
        jax.ShapeDtypeStruct((n, grid.slots, 3 * LANES), b16),
        jax.ShapeDtypeStruct((n, LANES, len(zone_list) * LANES), b16),
    ]
    scratch = [
        pltpu.VMEM((3, 3, 8, LANES), f32),
        pltpu.VMEM((3, 3, 8, LANES), f32),
        pltpu.VMEM((2 * grid.padded * ROWS, LANES), f32),
        pltpu.VMEM((2 * grid.padded * ROWS, LANES), f32),
        pltpu.VMEM((n, ROWS, 2 * LANES), f32),
        pltpu.VMEM((8, LANES), f32),
    ]
    params = pltpu.CompilerParams(vmem_limit_bytes=VMEM_LIMIT)

    def call(kernel, shapes, scratch, *values):
        return pl.pallas_call(kernel, out_shape=shapes, scratch_shapes=scratch, compiler_params=params)(*values)

    x, v, rest, flags, *rest_out = call(
        functools.partial(start_kernel, grid, layout), [cube, cube, plane, plane] + table_shapes + [forces], scratch, near, far
    )
    tables, force = rest_out[:5], rest_out[5]
    energies = jnp.zeros((8, LANES), f32)
    for step in range(ITERS):
        got = [from_ahead(force, (0, 0, by)) for by in range(1, grid.gz)]
        x, v, energies, force = call(
            functools.partial(step_kernel, grid, step),
            [cube, cube, small, forces],
            scratch,
            x, v, rest, flags, *tables, energies, force, *got,
        )
    got = [from_ahead(force, (0, 0, by)) for by in range(1, grid.gz)]
    speed, energies = call(
        functools.partial(last_kernel, grid), [jax.ShapeDtypeStruct((3, 8, LANES), f32), small], [], v, energies, force, *got
    )
    bead_total = 8 * clusters * grid.domains
    return (x[:, :8], speed, energies[:ITERS, :2] / bead_total)


def can_replicate(grid, positions, send_list, pair_list):
    return (
        grid.domains <= MAX_REPLICATED
        and grid.lists % 2 == 0
        and grid.gz == 2
        and positions.shape[2] == LANES
        and zone_sizes()[0] == LANES
        and pair_list.shape[1] % LANES == 0
        and sum(zone_sizes()) == send_list.shape[0]
        and send_list.shape[0] - LANES < LANES
    )


VMEM_LIMIT = 58 * 1024 * 1024


def solution(mesh):
    def on_any(positions, velocities, send_list, pair_list, constraint_flags):
        grid = Grid(mesh, pair_list.shape[1], send_list.shape[0])
        if can_replicate(grid, positions, send_list, pair_list):
            return replicated(grid, positions, velocities, send_list, pair_list, constraint_flags)
        return on_device(positions, velocities, send_list, pair_list, constraint_flags)

    return jax.shard_map(
        on_any,
        mesh=mesh,
        in_specs=(
            P(None, None, ("runs", "gx", "gy", "gz")),
            P(None, None, ("runs", "gx", "gy", "gz")),
            P(("runs", "gx", "gy", "gz")),
            P(None, ("runs", "gx", "gy", "gz")),
            P(None, ("runs", "gx", "gy", "gz")),
        ),
        out_specs=(
            P(None, None, ("runs", "gx", "gy", "gz")),
            P(None, None, ("runs", "gx", "gy", "gz")),
            P("runs", None),
        ),
        check_vma=False,
    )
```

```python
import functools

import jax
import jax.numpy as jnp
import numpy as np
from jax import lax
from jax.experimental import pallas as pl
from jax.experimental.pallas import tpu as pltpu
from jax.sharding import PartitionSpec as P

CX = 1
CY = 8
CZ = 16
ITERS = 3
NORDER = 4


time_step = 0.02
strength = 2.0
root_half = 0.7071067811865476
zone_list = ((1, 0, 0), (0, 1, 0), (0, 0, 1), (1, 1, 0), (1, 0, 1), (0, 1, 1), (1, 1, 1))


def from_behind(value, axis, by):
    count = lax.axis_size(axis)
    return lax.ppermute(value, axis, [(i, (i + by) % count) for i in range(count)])


def zone_sizes():
    return tuple(
        (
            (CX if direction[0] == 0 else 1)
            * (CY if direction[1] == 0 else 1)
            * (CZ if direction[2] == 0 else 1)
            for direction in zone_list
        )
    )


def split_blocks(packed, block_sizes):
    pieces = []
    position = 0
    for length in block_sizes:
        pieces.append(packed[:, :, position : position + length])
        position += length
    return pieces


def shell_offsets():
    block_sizes = zone_sizes()
    columns = []
    for number in range(7):
        direction = zone_list[number]
        column = np.array(
            [[direction[0] * CX], [direction[1] * CY], [direction[2] * CZ]], np.float32
        )
        columns.append(np.tile(column, (1, block_sizes[number])))
    return jnp.asarray(np.concatenate(columns, axis=1))[:, None, :]


def share_coords(coords, send_table):
    sizes_all = zone_sizes()
    chosen = jnp.dot(
        coords.reshape(24, -1), send_table, precision=lax.Precision.HIGHEST
    ).reshape(3, 8, -1)
    outgoing = split_blocks(chosen, sizes_all)
    along_y = from_behind(
        jnp.concatenate([outgoing[1], outgoing[3], outgoing[5], outgoing[6]], axis=2), "gy", -1
    )
    got_y = split_blocks(along_y, [sizes_all[1], sizes_all[3], sizes_all[5], sizes_all[6]])
    along_x = from_behind(
        jnp.concatenate([outgoing[0], outgoing[4], got_y[1], got_y[3]], axis=2), "gx", -1
    )
    got_x = split_blocks(along_x, [sizes_all[0], sizes_all[4], sizes_all[3], sizes_all[6]])
    along_z = from_behind(
        jnp.concatenate([outgoing[2], got_x[1], got_y[2], got_x[3]], axis=2), "gz", -1
    )
    got_z = split_blocks(along_z, [sizes_all[2], sizes_all[4], sizes_all[5], sizes_all[6]])
    received = [got_x[0], got_y[0], got_z[0], got_x[2], got_z[1], got_z[2], got_z[3]]
    return jnp.concatenate(received, axis=2) + shell_offsets()


def return_forces(halo_forces):
    sizes_all = zone_sizes()
    outgoing = split_blocks(halo_forces, sizes_all)
    along_z = from_behind(
        jnp.concatenate([outgoing[2], outgoing[4], outgoing[5], outgoing[6]], axis=2), "gz", 1
    )
    got_z = split_blocks(along_z, [sizes_all[2], sizes_all[4], sizes_all[5], sizes_all[6]])
    along_x = from_behind(
        jnp.concatenate([outgoing[0], outgoing[3], got_z[1], got_z[3]], axis=2), "gx", 1
    )
    got_x = split_blocks(along_x, [sizes_all[0], sizes_all[3], sizes_all[4], sizes_all[6]])
    settled = [got_x[0], got_z[0], got_x[2]]
    pending = [got_x[1], got_z[2], got_x[3]]
    along_y = from_behind(
        jnp.concatenate([outgoing[1], pending[0], pending[1], pending[2]], axis=2), "gy", 1
    )
    got_y = split_blocks(along_y, [sizes_all[1], sizes_all[3], sizes_all[5], sizes_all[6]])
    return jnp.concatenate(
        [settled[0], got_y[0], settled[1], got_y[1], settled[2], got_y[2], got_y[3]], axis=2
    )


def pair_tables(pair_list, extended_count):
    rows = lax.broadcasted_iota(jnp.int32, (extended_count, pair_list.shape[1]), 0)
    first_table = (rows == pair_list[0][None, :]).astype(jnp.float32)
    second_table = (rows == pair_list[1][None, :]).astype(jnp.float32)
    return (first_table, second_table)


def domain_forces(extended, pair_list, tables):
    extended_count = extended.shape[2]
    slot_count = pair_list.shape[1]
    first_ids = pair_list[0]
    second_ids = pair_list[1]
    flat = extended.reshape(24, extended_count)
    first_coords = jnp.dot(flat, tables[0], precision=lax.Precision.HIGHEST).reshape(
        3, 8, slot_count
    )
    second_coords = jnp.dot(flat, tables[1], precision=lax.Precision.HIGHEST).reshape(
        3, 8, slot_count
    )
    separation = first_coords[:, :, None, :] - second_coords[:, None, :, :]
    scaled = jnp.sum(separation * separation, axis=0)
    intersect = jnp.maximum(1.0 - scaled, 0.0)
    bead_row = lax.broadcasted_iota(jnp.int32, (8, 8, 1), 0)
    bead_column = lax.broadcasted_iota(jnp.int32, (8, 8, 1), 1)
    self_pair = (first_ids == second_ids)[None, None, :]
    usable = (first_ids < extended_count - 1)[None, None, :]
    weight = (jnp.where(self_pair, bead_row < bead_column, True) & usable).astype(jnp.float32)
    energy = strength * jnp.sum(weight * intersect * intersect * intersect)
    magnitude = 6.0 * strength * weight * intersect * intersect
    pushing = magnitude[None] * separation
    on_first = jnp.sum(pushing, axis=2).reshape(24, slot_count)
    on_second = (-jnp.sum(pushing, axis=1)).reshape(24, slot_count)
    contract = (((1,), (1,)), ((), ()))
    forces = lax.dot_general(on_first, tables[0], contract, precision=lax.Precision.HIGHEST)
    forces = forces + lax.dot_general(
        on_second, tables[1], contract, precision=lax.Precision.HIGHEST
    )
    return (forces.reshape(3, 8, extended_count), energy)


def local_forces(coords, send_table, pair_list, tables):
    halo_coords = share_coords(coords, send_table)
    dummy_cluster = jnp.zeros((3, 8, 1), jnp.float32)
    extended = jnp.concatenate([coords, halo_coords, dummy_cluster], axis=2)
    forces, energy = domain_forces(extended, pair_list, tables)
    cluster_count = coords.shape[2]
    returned = return_forces(forces[:, :, cluster_count : cluster_count + send_table.shape[1]])
    contract = (((1,), (1,)), ((), ()))
    added = lax.dot_general(
        returned.reshape(24, -1), send_table, contract, precision=lax.Precision.HIGHEST
    )
    home_forces = forces[:, :, :cluster_count] + added.reshape(3, 8, -1)
    return (home_forces, energy)


def link_vectors(coords):
    return coords[:, :-1, :] - coords[:, 1:, :]


def link_lengths(coords):
    vectors = link_vectors(coords)
    return jnp.sqrt(jnp.sum(vectors * vectors, axis=0))


def expand(coupling, source):
    coupling_down = jnp.pad(coupling, ((1, 0), (0, 0)))
    coupling_up = jnp.pad(coupling, ((0, 1), (0, 0)))
    series = source
    result = source
    for expansion in range(NORDER):
        series = (
            coupling_down * jnp.pad(series, ((1, 0), (0, 0)))[:-1]
            + coupling_up * jnp.pad(series, ((0, 1), (0, 0)))[1:]
        )
        result = result + series
    return result


def apply_links(coords, directions, solution):
    shifts = directions * (root_half * solution)[None]
    return (
        coords
        - jnp.pad(shifts, ((0, 0), (0, 1), (0, 0)))
        + jnp.pad(shifts, ((0, 0), (1, 0), (0, 0)))
    )


def constrain(previous, updated, rest_length, link_flags):
    old_vectors = link_vectors(previous)
    directions = (
        old_vectors / jnp.maximum(jnp.sqrt(jnp.sum(old_vectors * old_vectors, axis=0)), 0.2)[None]
    )
    coupling = (
        0.5
        * jnp.sum(directions[:, :-1] * directions[:, 1:], axis=0)
        * link_flags[:-1]
        * link_flags[1:]
    )
    projected = jnp.sum(directions * link_vectors(updated), axis=0)
    solution = expand(coupling, link_flags * root_half * (projected - rest_length))
    updated = apply_links(updated, directions, solution)
    vectors = link_vectors(updated)
    squared = jnp.sum(vectors * vectors, axis=0)
    target = jnp.sqrt(
        jnp.maximum(2.0 * rest_length * rest_length - squared, 0.25 * rest_length * rest_length)
    )
    solution = expand(coupling, link_flags * root_half * (rest_length - target))
    updated = apply_links(updated, directions, solution)
    return updated


def total_over(value, axis):
    count = lax.axis_size(axis)
    if count > 4:
        return lax.psum(value, axis)
    total = value
    for by in range(1, count):
        total = total + from_behind(value, axis, by)
    return total


def on_device(positions, velocities, send_list, pair_list, constraint_flags):
    link_flags = constraint_flags.astype(jnp.float32)
    rest_length = link_lengths(positions)
    bead_total = 8 * positions.shape[2] * lax.axis_size(("gx", "gy", "gz"))
    tables = pair_tables(pair_list, positions.shape[2] + send_list.shape[0] + 1)
    owned = lax.broadcasted_iota(jnp.int32, (positions.shape[2], send_list.shape[0]), 0)
    send_table = (owned == send_list[None, :]).astype(jnp.float32)
    forces, potential = local_forces(positions, send_table, pair_list, tables)
    energy_rows = []
    for iteration in range(ITERS):
        half_speed = velocities + 0.5 * time_step * forces
        updated = constrain(positions, positions + time_step * half_speed, rest_length, link_flags)
        half_speed = (updated - positions) / time_step
        forces, potential = local_forces(updated, send_table, pair_list, tables)
        velocities = half_speed + 0.5 * time_step * forces
        positions = updated
        kinetic = 0.5 * jnp.sum(velocities * velocities)
        energy_rows.append(jnp.stack([potential, kinetic]))
    energies = jnp.stack(energy_rows)
    for axis in ("gz", "gy", "gx"):
        energies = total_over(energies, axis)
    return (positions, velocities, energies / bead_total)


LANES = 128
ROWS = 24
MAX_REPLICATED = 16


def split_rows(value):
    high = value.astype(jnp.bfloat16).astype(jnp.float32)
    return jnp.concatenate([high, value - high], axis=0).astype(jnp.bfloat16)


def joined(value):
    return value[:ROWS] + value[ROWS:]


class Grid:
    def __init__(self, mesh, slot_count, halo_count):
        self.gx, self.gy, self.gz = (mesh.shape[a] for a in ("gx", "gy", "gz"))
        self.domains = self.gx * self.gy * self.gz
        self.lists = self.gx * self.gy
        self.blocks = slot_count // LANES
        self.padded = (self.blocks + 7) // 8 * 8
        self.dummy = LANES + halo_count
        self.slots = 2 * self.blocks * LANES
        sizes = zone_sizes()
        self.zones = []
        start = 0
        for direction, size in zip(zone_list[1:], sizes[1:]):
            self.zones.append((direction, start, start + size))
            start += size

    def domain(self, i, j, direction):
        i = lax.rem(i + direction[0], self.gx) if not isinstance(i, int) else (i + direction[0]) % self.gx
        j = lax.rem(j + direction[1], self.gy) if not isinstance(j, int) else (j + direction[1]) % self.gy
        return (i * self.gy + j) * self.gz + direction[2] % self.gz

    def rows_of(self, i, j, direction):
        row = self.domain(i, j, direction) * 8
        return pl.ds(row if isinstance(row, int) else pl.multiple_of(row, 8), 8)


def lanes_of(shape):
    return lax.broadcasted_iota(jnp.int32, shape, 1)


def take_lanes(source, index):
    return jnp.take_along_axis(source, index, axis=1, mode="promise_in_bounds")


def build_tables(grid, near_ref, far_ref, pair_row, send_row, ids_ref, weight_ref, index_ref, table_ref, zone_ref):
    blocks = grid.blocks
    lane = lanes_of((8, LANES))
    own_code = lanes_of((LANES, LANES)).astype(jnp.float32).astype(jnp.bfloat16)
    first_code = (lanes_of((LANES, LANES)) + LANES).astype(jnp.float32).astype(jnp.bfloat16)
    rest_code = (-1 - lanes_of((LANES, LANES))).astype(jnp.float32).astype(jnp.bfloat16)
    one = jnp.ones((LANES, LANES), jnp.bfloat16)
    zero = jnp.zeros((LANES, LANES), jnp.bfloat16)

    def send_of(number, row):
        source = near_ref if number % grid.gz == 0 else far_ref
        return source[number // grid.gz, pl.ds(send_row + row, 1), :]

    for number in range(grid.lists):
        i, j = number // grid.gy, number % grid.gy
        to_x = send_of(grid.domain(i, j, zone_list[0]), 0)
        rest = jnp.zeros((1, LANES), jnp.float32)
        for direction, start, stop in grid.zones:
            row = send_of(grid.domain(i, j, direction), 1)
            rest = jnp.where((lane[:1] >= start) & (lane[:1] < stop), row, rest)
        both = jnp.concatenate([to_x, rest] + [jnp.zeros((6, LANES), jnp.float32)], axis=0)
        index_ref[number] = both.astype(jnp.int32)

    def one_list(number, carry):
        first = near_ref[number, pl.ds(pair_row, blocks), :]
        second = near_ref[number, pl.ds(pair_row + blocks, blocks), :]
        fill = jnp.full((grid.padded - blocks, LANES), float(grid.dummy), jnp.float32)
        parts = [[first, fill], [second, fill]] if grid.padded > blocks else [[first], [second]]
        first, second = (jnp.concatenate(p, axis=0) for p in parts)
        ids_ref[0, number] = first.astype(jnp.int32)
        ids_ref[1, number] = second.astype(jnp.int32)
        usable = jnp.where(first < float(grid.dummy), 1.0, 0.0)
        weight_ref[number] = jnp.where(first == second, 0.5, 1.0) * usable
        both = index_ref[number].astype(jnp.float32)
        codes = jnp.concatenate([first, second], axis=0)
        codes = jnp.where(codes < 2.0 * LANES, codes, 2.0 * LANES - 1.0 - codes)
        turned = jnp.transpose(jnp.concatenate([codes, both], axis=0))
        for side in range(2):
            for block in range(blocks):
                at = side * grid.padded + block
                column = jnp.broadcast_to(turned[:, at : at + 1], (LANES, LANES)).astype(jnp.bfloat16)
                rows = pl.ds((side * blocks + block) * LANES, LANES)
                for part, code in enumerate((own_code, first_code, rest_code)):
                    table_ref[number, rows, pl.ds(part * LANES, LANES)] = jnp.where(column == code, one, zero)
        at = 2 * grid.padded
        column = jnp.broadcast_to(turned[:, at : at + 1], (LANES, LANES)).astype(jnp.bfloat16)
        zone_ref[number, :, pl.ds(0, LANES)] = jnp.where(column == own_code, one, zero)
        column = jnp.broadcast_to(turned[:, at + 1 : at + 2], (LANES, LANES)).astype(jnp.bfloat16)
        slot = lax.broadcasted_iota(jnp.int32, (LANES, LANES), 0).astype(jnp.float32).astype(jnp.bfloat16)
        for part, (direction, start, stop) in enumerate(grid.zones):
            here = (column == own_code) & (slot >= start) & (slot < stop)
            zone_ref[number, :, pl.ds((part + 1) * LANES, LANES)] = jnp.where(here, one, zero)
        return carry

    lax.fori_loop(0, grid.lists, one_list, 0)


def gather_and_push(grid, number, x_ref, ids_ref, weight_ref, index_ref, ext_ref, push_ref, energy_ref):
    i, j = lax.div(number, grid.gy), lax.rem(number, grid.gy)
    lane = lanes_of((8, LANES))
    cell = (CX, CY, CZ)
    to_x = jnp.broadcast_to(index_ref[number, pl.ds(0, 1), :], (8, LANES))
    rest = jnp.broadcast_to(index_ref[number, pl.ds(1, 1), :], (8, LANES))
    for c in range(3):
        ext_ref[c, 0] = x_ref[c, grid.rows_of(i, j, (0, 0, 0)), :]
        shift = float(zone_list[0][c] * cell[c])
        ext_ref[c, 1] = take_lanes(x_ref[c, grid.rows_of(i, j, zone_list[0]), :], to_x) + shift
        value = jnp.zeros((8, LANES), jnp.float32)
        for direction, start, stop in grid.zones:
            shift = float(direction[c] * cell[c])
            got = take_lanes(x_ref[c, grid.rows_of(i, j, direction), :], rest) + shift
            value = jnp.where((lane >= start) & (lane < stop), got, value)
        ext_ref[c, 2] = value
    for group in range(grid.padded // 8):
        sides = []
        for side in range(2):
            ids = ids_ref[side, number, pl.ds(8 * group, 8), :]
            low = ids & (LANES - 1)
            in_own = ids < LANES
            in_first = ids < 2 * LANES
            coords = []
            for c in range(3):
                line = []
                for bead in range(8):
                    a, b, d = (
                        take_lanes(jnp.broadcast_to(ext_ref[c, part, pl.ds(bead, 1), :], (8, LANES)), low)
                        for part in range(3)
                    )
                    line.append(jnp.where(in_own, a, jnp.where(in_first, b, d)))
                coords.append(line)
            sides.append(coords)
        weight = weight_ref[number, pl.ds(8 * group, 8), :]
        scale = weight * (6.0 * strength)
        energy = None
        on_second = [[None] * 8 for _ in range(3)]
        for k in range(8):
            on_first = [None] * 3
            for l in range(8):
                apart = [sides[0][c][k] - sides[1][c][l] for c in range(3)]
                scaled = apart[0] * apart[0] + apart[1] * apart[1] + apart[2] * apart[2]
                intersect = jnp.maximum(1.0 - scaled, 0.0)
                square = intersect * intersect
                cube = square * intersect
                energy = cube if energy is None else energy + cube
                for c in range(3):
                    pushing = square * apart[c]
                    on_first[c] = pushing if l == 0 else on_first[c] + pushing
                    on_second[c][l] = pushing if k == 0 else on_second[c][l] + pushing
            for c in range(3):
                row = (8 * group) * ROWS + c * 8 + k
                push_ref[pl.ds(row, 8, stride=ROWS), :] = on_first[c] * scale
        for c in range(3):
            for l in range(8):
                row = (grid.padded + 8 * group) * ROWS + c * 8 + l
                push_ref[pl.ds(row, 8, stride=ROWS), :] = -(on_second[c][l] * scale)
        own_beads = jnp.where(weight == 0.5, 8.0, 0.0)
        energy_ref[...] += strength * weight * (energy - own_beads)


def scatter(grid, number, push_ref, table_ref, force_ref, halo_ref):
    pieces = []
    for side in range(2):
        for block in range(grid.blocks):
            pieces.append(push_ref[pl.ds((side * grid.padded + block) * ROWS, ROWS), :])
    pushes = split_rows(jnp.concatenate(pieces, axis=1))
    sums = joined(jnp.dot(pushes, table_ref[number], preferred_element_type=jnp.float32))
    row = pl.multiple_of(number * grid.gz * 8, 8)
    for c in range(3):
        force_ref[pl.ds(c * grid.domains * 8 + row, 8), :] = sums[8 * c : 8 * c + 8, :LANES]
    halo_ref[number] = sums[:, LANES:]


def pair_forces(grid, x_ref, tables, force_ref, scratch):
    ids_ref, weight_ref, index_ref, table_ref, zone_ref = tables
    ext_a, ext_b, push_a, push_b, halo_ref, energy_ref = scratch
    force_ref[...] = jnp.zeros(force_ref.shape, jnp.float32)
    energy_ref[...] = jnp.zeros((8, LANES), jnp.float32)

    def forward(number, ext_ref, push_ref):
        gather_and_push(grid, number, x_ref, ids_ref, weight_ref, index_ref, ext_ref, push_ref, energy_ref)

    def back(number, push_ref):
        scatter(grid, number, push_ref, table_ref, force_ref, halo_ref)

    forward(0, ext_a, push_a)

    def two(m, carry):
        back(2 * m, push_a)
        forward(2 * m + 1, ext_b, push_b)
        back(2 * m + 1, push_b)
        forward(2 * m + 2, ext_a, push_a)
        return carry

    lax.fori_loop(0, grid.lists // 2 - 1, two, 0)
    back(grid.lists - 2, push_a)
    forward(grid.lists - 1, ext_b, push_b)
    back(grid.lists - 1, push_b)
    for number in range(grid.lists):
        i, j = number // grid.gy, number % grid.gy
        halo = halo_ref[number]
        to_x = joined(
            jnp.dot(split_rows(halo[:, :LANES]), zone_ref[number, :, pl.ds(0, LANES)], preferred_element_type=jnp.float32)
        )
        rest = joined(
            jnp.dot(
                split_rows(halo[:, LANES:]),
                zone_ref[number, :, pl.ds(LANES, len(grid.zones) * LANES)],
                preferred_element_type=jnp.float32,
            )
        )
        targets = [(zone_list[0], to_x)]
        for part, (direction, start, stop) in enumerate(grid.zones):
            targets.append((direction, rest[:, part * LANES : (part + 1) * LANES]))
        for direction, value in targets:
            row = grid.domain(i, j, direction) * 8
            for c in range(3):
                force_ref[pl.ds(c * grid.domains * 8 + row, 8), :] += value[8 * c : 8 * c + 8]
    force_ref[pl.ds(3 * grid.domains * 8, 8), :] = energy_ref[...]


def start_kernel(grid, layout, near_ref, far_ref, *refs):
    x_ref, v_ref, rest_ref, flag_ref, ids_ref, weight_ref, index_ref, table_ref, zone_ref, force_ref = refs[:10]
    scratch = refs[10:]
    for number in range(grid.domains):
        source = near_ref if number % grid.gz == 0 else far_ref
        at = number // grid.gz
        rows = pl.ds(number * 8, 8)
        for c in range(3):
            x_ref[c, rows, :] = source[at, pl.ds(layout["positions"] + 8 * c, 8), :]
            v_ref[c, rows, :] = source[at, pl.ds(layout["velocities"] + 8 * c, 8), :]
        flag_ref[rows, :] = source[at, pl.ds(layout["flags"], 8), :]
    rest_ref[...] = link_length([x_ref[c] for c in range(3)])
    build_tables(grid, near_ref, far_ref, layout["pairs"], layout["sends"], ids_ref, weight_ref, index_ref, table_ref, zone_ref)
    pair_forces(grid, x_ref, (ids_ref, weight_ref, index_ref, table_ref, zone_ref), force_ref, scratch)


def up(value):
    return pltpu.roll(value, value.shape[0] - 1, 0)


def down(value):
    return pltpu.roll(value, 1, 0)


def dot3(a, b):
    return a[0] * b[0] + a[1] * b[1] + a[2] * b[2]


def links_of(x):
    return [c - up(c) for c in x]


def link_length(x):
    vectors = links_of(x)
    return jnp.sqrt(dot3(vectors, vectors))


def expand_rows(coupling, before, source):
    series = source
    result = source
    for expansion in range(NORDER):
        series = before * down(series) + coupling * up(series)
        result = result + series
    return result


def apply_rows(x, directions, solution):
    moved = []
    for c in range(3):
        shift = directions[c] * (root_half * solution)
        moved.append(x[c] - shift + down(shift))
    return moved


def constrain_rows(previous, updated, rest, flags):
    old = links_of(previous)
    length = jnp.maximum(jnp.sqrt(dot3(old, old)), 0.2)
    directions = [c / length for c in old]
    coupling = 0.5 * dot3(directions, [up(c) for c in directions]) * flags * up(flags)
    before = down(coupling)
    projected = dot3(directions, links_of(updated))
    solution = expand_rows(coupling, before, flags * (root_half * (projected - rest)))
    updated = apply_rows(updated, directions, solution)
    vectors = links_of(updated)
    squared = dot3(vectors, vectors)
    target = jnp.sqrt(jnp.maximum(2.0 * rest * rest - squared, 0.25 * rest * rest))
    solution = expand_rows(coupling, before, flags * (root_half * (rest - target)))
    return apply_rows(updated, directions, solution)


def total_force(grid, own_ref, got_refs):
    size = grid.domains * 8
    total = []
    for c in range(3):
        pieces = []
        for number in range(grid.domains):
            base, k = number // grid.gz * grid.gz, number % grid.gz
            value = own_ref[pl.ds(c * size + number * 8, 8), :]
            for by, ref in enumerate(got_refs, 1):
                value = value + ref[pl.ds(c * size + (base + (k - by) % grid.gz) * 8, 8), :]
            pieces.append(value)
        total.append(jnp.concatenate(pieces, axis=0))
    return total


def energy_row(grid, own_ref, got_refs, v, row, previous):
    rows = pl.ds(3 * grid.domains * 8, 8)
    potential = own_ref[rows, :]
    for ref in got_refs:
        potential = potential + ref[rows, :]
    kinetic = 0.5 * dot3(v, v)
    lane = lanes_of((8, LANES))
    at = lax.broadcasted_iota(jnp.int32, (8, LANES), 0) == row
    previous = jnp.where(at & (lane == 0), jnp.sum(potential), previous)
    return jnp.where(at & (lane == 1), jnp.sum(kinetic), previous)


def step_kernel(grid, step, x_ref, v_ref, rest_ref, flag_ref, ids_ref, weight_ref, index_ref, table_ref, zone_ref, energies_ref, own_ref, *refs):
    got_refs, refs = refs[: grid.gz - 1], refs[grid.gz - 1 :]
    moved_ref, half_ref, energy_out_ref, force_ref = refs[:4]
    scratch = refs[4:]
    force = total_force(grid, own_ref, got_refs)
    x = [x_ref[c] for c in range(3)]
    v = [v_ref[c] for c in range(3)]
    if step > 0:
        v = [v[c] + (0.5 * time_step) * force[c] for c in range(3)]
        energy_out_ref[...] = energy_row(grid, own_ref, got_refs, v, step - 1, energies_ref[...])
    else:
        energy_out_ref[...] = energies_ref[...]
    half = [v[c] + (0.5 * time_step) * force[c] for c in range(3)]
    moved = constrain_rows(x, [x[c] + time_step * half[c] for c in range(3)], rest_ref[...], flag_ref[...])
    for c in range(3):
        moved_ref[c] = moved[c]
        half_ref[c] = (moved[c] - x[c]) / time_step
    pair_forces(grid, moved_ref, (ids_ref, weight_ref, index_ref, table_ref, zone_ref), force_ref, scratch)


def last_kernel(grid, v_ref, energies_ref, own_ref, *refs):
    got_refs, (speed_ref, energy_out_ref) = refs[: grid.gz - 1], refs[grid.gz - 1 :]
    force = total_force(grid, own_ref, got_refs)
    v = [v_ref[c] + (0.5 * time_step) * force[c] for c in range(3)]
    for c in range(3):
        speed_ref[c] = v[c][:8]
    energy_out_ref[...] = energy_row(grid, own_ref, got_refs, v, ITERS - 1, energies_ref[...])


def from_ahead(value, steps):
    names = [a for a, by in zip(("gx", "gy", "gz"), steps) if by]
    if not names:
        return value
    counts = [lax.axis_size(a) for a in names]
    pairs = []
    for target in np.ndindex(*counts):
        source = [(t + by) % n for t, by, n in zip(target, [s for s in steps if s], counts)]
        pairs.append(tuple(int(np.ravel_multi_index(p, counts)) for p in (source, target)))
    return lax.ppermute(value, tuple(names), pairs)


def replicated(grid, positions, velocities, send_list, pair_list, constraint_flags):
    clusters = positions.shape[2]
    sends = jnp.pad(send_list, (0, -send_list.shape[0] % LANES)).reshape(-1, LANES)
    parts = dict(
        positions=positions.reshape(ROWS, clusters),
        velocities=velocities.reshape(ROWS, clusters),
        flags=jnp.pad(constraint_flags.astype(jnp.float32), ((0, 1), (0, 0))),
        pairs=pair_list.astype(jnp.float32).reshape(-1, LANES),
        sends=sends.astype(jnp.float32),
    )
    layout, row = {}, 0
    for name, value in parts.items():
        layout[name] = row
        row += value.shape[0]
    pack = jnp.concatenate(list(parts.values()) + [jnp.zeros((-row % 8, LANES), jnp.float32)], axis=0)
    near = jnp.stack([from_ahead(pack, (i, j, 0)) for i in range(grid.gx) for j in range(grid.gy)])
    far = from_ahead(near, (0, 0, 1))
    f32, i32, b16 = jnp.float32, jnp.int32, jnp.bfloat16
    n, rows = grid.lists, grid.domains * 8
    cube = jax.ShapeDtypeStruct((3, rows, LANES), f32)
    plane = jax.ShapeDtypeStruct((rows, LANES), f32)
    small = jax.ShapeDtypeStruct((8, LANES), f32)
    forces = jax.ShapeDtypeStruct((3 * rows + 8, LANES), f32)
    table_shapes = [
        jax.ShapeDtypeStruct((2, n, grid.padded, LANES), i32),
        jax.ShapeDtypeStruct((n, grid.padded, LANES), f32),
        jax.ShapeDtypeStruct((n, 8, LANES), i32),
        jax.ShapeDtypeStruct((n, grid.slots, 3 * LANES), b16),
        jax.ShapeDtypeStruct((n, LANES, len(zone_list) * LANES), b16),
    ]
    scratch = [
        pltpu.VMEM((3, 3, 8, LANES), f32),
        pltpu.VMEM((3, 3, 8, LANES), f32),
        pltpu.VMEM((2 * grid.padded * ROWS, LANES), f32),
        pltpu.VMEM((2 * grid.padded * ROWS, LANES), f32),
        pltpu.VMEM((n, ROWS, 2 * LANES), f32),
        pltpu.VMEM((8, LANES), f32),
    ]
    params = pltpu.CompilerParams(vmem_limit_bytes=VMEM_LIMIT)

    def call(kernel, shapes, scratch, *values):
        return pl.pallas_call(kernel, out_shape=shapes, scratch_shapes=scratch, compiler_params=params)(*values)

    x, v, rest, flags, *rest_out = call(
        functools.partial(start_kernel, grid, layout), [cube, cube, plane, plane] + table_shapes + [forces], scratch, near, far
    )
    tables, force = rest_out[:5], rest_out[5]
    energies = jnp.zeros((8, LANES), f32)
    for step in range(ITERS):
        got = [from_ahead(force, (0, 0, by)) for by in range(1, grid.gz)]
        x, v, energies, force = call(
            functools.partial(step_kernel, grid, step),
            [cube, cube, small, forces],
            scratch,
            x, v, rest, flags, *tables, energies, force, *got,
        )
    got = [from_ahead(force, (0, 0, by)) for by in range(1, grid.gz)]
    speed, energies = call(
        functools.partial(last_kernel, grid), [jax.ShapeDtypeStruct((3, 8, LANES), f32), small], [], v, energies, force, *got
    )
    bead_total = 8 * clusters * grid.domains
    return (x[:, :8], speed, energies[:ITERS, :2] / bead_total)


def can_replicate(grid, positions, send_list, pair_list):
    return (
        grid.domains <= MAX_REPLICATED
        and grid.lists % 2 == 0
        and grid.gz == 2
        and positions.shape[2] == LANES
        and zone_sizes()[0] == LANES
        and pair_list.shape[1] % LANES == 0
        and sum(zone_sizes()) == send_list.shape[0]
        and send_list.shape[0] - LANES < LANES
    )


VMEM_LIMIT = 16 * 1024 * 1024


def solution(mesh):
    def on_any(positions, velocities, send_list, pair_list, constraint_flags):
        grid = Grid(mesh, pair_list.shape[1], send_list.shape[0])
        if can_replicate(grid, positions, send_list, pair_list):
            return replicated(grid, positions, velocities, send_list, pair_list, constraint_flags)
        return on_device(positions, velocities, send_list, pair_list, constraint_flags)

    return jax.shard_map(
        on_any,
        mesh=mesh,
        in_specs=(
            P(None, None, ("runs", "gx", "gy", "gz")),
            P(None, None, ("runs", "gx", "gy", "gz")),
            P(("runs", "gx", "gy", "gz")),
            P(None, ("runs", "gx", "gy", "gz")),
            P(None, ("runs", "gx", "gy", "gz")),
        ),
        out_specs=(
            P(None, None, ("runs", "gx", "gy", "gz")),
            P(None, None, ("runs", "gx", "gy", "gz")),
            P("runs", None),
        ),
        check_vma=False,
    )
```

```python
import functools

import jax
import jax.numpy as jnp
import numpy as np
from jax import lax
from jax.experimental import pallas as pl
from jax.experimental.pallas import tpu as pltpu
from jax.sharding import PartitionSpec as P

CX = 1
CY = 8
CZ = 16
ITERS = 3
NORDER = 4


time_step = 0.02
strength = 2.0
root_half = 0.7071067811865476
zone_list = ((1, 0, 0), (0, 1, 0), (0, 0, 1), (1, 1, 0), (1, 0, 1), (0, 1, 1), (1, 1, 1))


def from_behind(value, axis, by):
    count = lax.axis_size(axis)
    return lax.ppermute(value, axis, [(i, (i + by) % count) for i in range(count)])


def zone_sizes():
    return tuple(
        (
            (CX if direction[0] == 0 else 1)
            * (CY if direction[1] == 0 else 1)
            * (CZ if direction[2] == 0 else 1)
            for direction in zone_list
        )
    )


def split_blocks(packed, block_sizes):
    pieces = []
    position = 0
    for length in block_sizes:
        pieces.append(packed[:, :, position : position + length])
        position += length
    return pieces


def shell_offsets():
    block_sizes = zone_sizes()
    columns = []
    for number in range(7):
        direction = zone_list[number]
        column = np.array(
            [[direction[0] * CX], [direction[1] * CY], [direction[2] * CZ]], np.float32
        )
        columns.append(np.tile(column, (1, block_sizes[number])))
    return jnp.asarray(np.concatenate(columns, axis=1))[:, None, :]


def share_coords(coords, send_table):
    sizes_all = zone_sizes()
    chosen = jnp.dot(
        coords.reshape(24, -1), send_table, precision=lax.Precision.HIGHEST
    ).reshape(3, 8, -1)
    outgoing = split_blocks(chosen, sizes_all)
    along_y = from_behind(
        jnp.concatenate([outgoing[1], outgoing[3], outgoing[5], outgoing[6]], axis=2), "gy", -1
    )
    got_y = split_blocks(along_y, [sizes_all[1], sizes_all[3], sizes_all[5], sizes_all[6]])
    along_x = from_behind(
        jnp.concatenate([outgoing[0], outgoing[4], got_y[1], got_y[3]], axis=2), "gx", -1
    )
    got_x = split_blocks(along_x, [sizes_all[0], sizes_all[4], sizes_all[3], sizes_all[6]])
    along_z = from_behind(
        jnp.concatenate([outgoing[2], got_x[1], got_y[2], got_x[3]], axis=2), "gz", -1
    )
    got_z = split_blocks(along_z, [sizes_all[2], sizes_all[4], sizes_all[5], sizes_all[6]])
    received = [got_x[0], got_y[0], got_z[0], got_x[2], got_z[1], got_z[2], got_z[3]]
    return jnp.concatenate(received, axis=2) + shell_offsets()


def return_forces(halo_forces):
    sizes_all = zone_sizes()
    outgoing = split_blocks(halo_forces, sizes_all)
    along_z = from_behind(
        jnp.concatenate([outgoing[2], outgoing[4], outgoing[5], outgoing[6]], axis=2), "gz", 1
    )
    got_z = split_blocks(along_z, [sizes_all[2], sizes_all[4], sizes_all[5], sizes_all[6]])
    along_x = from_behind(
        jnp.concatenate([outgoing[0], outgoing[3], got_z[1], got_z[3]], axis=2), "gx", 1
    )
    got_x = split_blocks(along_x, [sizes_all[0], sizes_all[3], sizes_all[4], sizes_all[6]])
    settled = [got_x[0], got_z[0], got_x[2]]
    pending = [got_x[1], got_z[2], got_x[3]]
    along_y = from_behind(
        jnp.concatenate([outgoing[1], pending[0], pending[1], pending[2]], axis=2), "gy", 1
    )
    got_y = split_blocks(along_y, [sizes_all[1], sizes_all[3], sizes_all[5], sizes_all[6]])
    return jnp.concatenate(
        [settled[0], got_y[0], settled[1], got_y[1], settled[2], got_y[2], got_y[3]], axis=2
    )


def pair_tables(pair_list, extended_count):
    rows = lax.broadcasted_iota(jnp.int32, (extended_count, pair_list.shape[1]), 0)
    first_table = (rows == pair_list[0][None, :]).astype(jnp.float32)
    second_table = (rows == pair_list[1][None, :]).astype(jnp.float32)
    return (first_table, second_table)


def domain_forces(extended, pair_list, tables):
    extended_count = extended.shape[2]
    slot_count = pair_list.shape[1]
    first_ids = pair_list[0]
    second_ids = pair_list[1]
    flat = extended.reshape(24, extended_count)
    first_coords = jnp.dot(flat, tables[0], precision=lax.Precision.HIGHEST).reshape(
        3, 8, slot_count
    )
    second_coords = jnp.dot(flat, tables[1], precision=lax.Precision.HIGHEST).reshape(
        3, 8, slot_count
    )
    separation = first_coords[:, :, None, :] - second_coords[:, None, :, :]
    scaled = jnp.sum(separation * separation, axis=0)
    intersect = jnp.maximum(1.0 - scaled, 0.0)
    bead_row = lax.broadcasted_iota(jnp.int32, (8, 8, 1), 0)
    bead_column = lax.broadcasted_iota(jnp.int32, (8, 8, 1), 1)
    self_pair = (first_ids == second_ids)[None, None, :]
    usable = (first_ids < extended_count - 1)[None, None, :]
    weight = (jnp.where(self_pair, bead_row < bead_column, True) & usable).astype(jnp.float32)
    energy = strength * jnp.sum(weight * intersect * intersect * intersect)
    magnitude = 6.0 * strength * weight * intersect * intersect
    pushing = magnitude[None] * separation
    on_first = jnp.sum(pushing, axis=2).reshape(24, slot_count)
    on_second = (-jnp.sum(pushing, axis=1)).reshape(24, slot_count)
    contract = (((1,), (1,)), ((), ()))
    forces = lax.dot_general(on_first, tables[0], contract, precision=lax.Precision.HIGHEST)
    forces = forces + lax.dot_general(
        on_second, tables[1], contract, precision=lax.Precision.HIGHEST
    )
    return (forces.reshape(3, 8, extended_count), energy)


def local_forces(coords, send_table, pair_list, tables):
    halo_coords = share_coords(coords, send_table)
    dummy_cluster = jnp.zeros((3, 8, 1), jnp.float32)
    extended = jnp.concatenate([coords, halo_coords, dummy_cluster], axis=2)
    forces, energy = domain_forces(extended, pair_list, tables)
    cluster_count = coords.shape[2]
    returned = return_forces(forces[:, :, cluster_count : cluster_count + send_table.shape[1]])
    contract = (((1,), (1,)), ((), ()))
    added = lax.dot_general(
        returned.reshape(24, -1), send_table, contract, precision=lax.Precision.HIGHEST
    )
    home_forces = forces[:, :, :cluster_count] + added.reshape(3, 8, -1)
    return (home_forces, energy)


def link_vectors(coords):
    return coords[:, :-1, :] - coords[:, 1:, :]


def link_lengths(coords):
    vectors = link_vectors(coords)
    return jnp.sqrt(jnp.sum(vectors * vectors, axis=0))


def expand(coupling, source):
    coupling_down = jnp.pad(coupling, ((1, 0), (0, 0)))
    coupling_up = jnp.pad(coupling, ((0, 1), (0, 0)))
    series = source
    result = source
    for expansion in range(NORDER):
        series = (
            coupling_down * jnp.pad(series, ((1, 0), (0, 0)))[:-1]
            + coupling_up * jnp.pad(series, ((0, 1), (0, 0)))[1:]
        )
        result = result + series
    return result


def apply_links(coords, directions, solution):
    shifts = directions * (root_half * solution)[None]
    return (
        coords
        - jnp.pad(shifts, ((0, 0), (0, 1), (0, 0)))
        + jnp.pad(shifts, ((0, 0), (1, 0), (0, 0)))
    )


def constrain(previous, updated, rest_length, link_flags):
    old_vectors = link_vectors(previous)
    directions = (
        old_vectors / jnp.maximum(jnp.sqrt(jnp.sum(old_vectors * old_vectors, axis=0)), 0.2)[None]
    )
    coupling = (
        0.5
        * jnp.sum(directions[:, :-1] * directions[:, 1:], axis=0)
        * link_flags[:-1]
        * link_flags[1:]
    )
    projected = jnp.sum(directions * link_vectors(updated), axis=0)
    solution = expand(coupling, link_flags * root_half * (projected - rest_length))
    updated = apply_links(updated, directions, solution)
    vectors = link_vectors(updated)
    squared = jnp.sum(vectors * vectors, axis=0)
    target = jnp.sqrt(
        jnp.maximum(2.0 * rest_length * rest_length - squared, 0.25 * rest_length * rest_length)
    )
    solution = expand(coupling, link_flags * root_half * (rest_length - target))
    updated = apply_links(updated, directions, solution)
    return updated


def total_over(value, axis):
    count = lax.axis_size(axis)
    if count > 4:
        return lax.psum(value, axis)
    total = value
    for by in range(1, count):
        total = total + from_behind(value, axis, by)
    return total


def on_device(positions, velocities, send_list, pair_list, constraint_flags):
    link_flags = constraint_flags.astype(jnp.float32)
    rest_length = link_lengths(positions)
    bead_total = 8 * positions.shape[2] * lax.axis_size(("gx", "gy", "gz"))
    tables = pair_tables(pair_list, positions.shape[2] + send_list.shape[0] + 1)
    owned = lax.broadcasted_iota(jnp.int32, (positions.shape[2], send_list.shape[0]), 0)
    send_table = (owned == send_list[None, :]).astype(jnp.float32)
    forces, potential = local_forces(positions, send_table, pair_list, tables)
    energy_rows = []
    for iteration in range(ITERS):
        half_speed = velocities + 0.5 * time_step * forces
        updated = constrain(positions, positions + time_step * half_speed, rest_length, link_flags)
        half_speed = (updated - positions) / time_step
        forces, potential = local_forces(updated, send_table, pair_list, tables)
        velocities = half_speed + 0.5 * time_step * forces
        positions = updated
        kinetic = 0.5 * jnp.sum(velocities * velocities)
        energy_rows.append(jnp.stack([potential, kinetic]))
    energies = jnp.stack(energy_rows)
    for axis in ("gz", "gy", "gx"):
        energies = total_over(energies, axis)
    return (positions, velocities, energies / bead_total)


LANES = 128
ROWS = 24
MAX_REPLICATED = 16


def split_rows(value):
    high = value.astype(jnp.bfloat16).astype(jnp.float32)
    return jnp.concatenate([high, value - high], axis=0).astype(jnp.bfloat16)


def joined(value):
    return value[:ROWS] + value[ROWS:]


class Grid:
    def __init__(self, mesh, slot_count, halo_count):
        self.gx, self.gy, self.gz = (mesh.shape[a] for a in ("gx", "gy", "gz"))
        self.domains = self.gx * self.gy * self.gz
        self.lists = self.gx * self.gy
        self.blocks = slot_count // LANES
        self.padded = (self.blocks + 7) // 8 * 8
        self.dummy = LANES + halo_count
        self.slots = 2 * self.blocks * LANES
        sizes = zone_sizes()
        self.zones = []
        start = 0
        for direction, size in zip(zone_list[1:], sizes[1:]):
            self.zones.append((direction, start, start + size))
            start += size

    def domain(self, i, j, direction):
        i = lax.rem(i + direction[0], self.gx) if not isinstance(i, int) else (i + direction[0]) % self.gx
        j = lax.rem(j + direction[1], self.gy) if not isinstance(j, int) else (j + direction[1]) % self.gy
        return (i * self.gy + j) * self.gz + direction[2] % self.gz

    def rows_of(self, i, j, direction):
        row = self.domain(i, j, direction) * 8
        return pl.ds(row if isinstance(row, int) else pl.multiple_of(row, 8), 8)


def lanes_of(shape):
    return lax.broadcasted_iota(jnp.int32, shape, 1)


def take_lanes(source, index):
    return jnp.take_along_axis(source, index, axis=1, mode="promise_in_bounds")


def build_tables(grid, near_ref, far_ref, pair_row, send_row, ids_ref, weight_ref, index_ref, table_ref, zone_ref):
    blocks = grid.blocks
    lane = lanes_of((8, LANES))
    own_code = lanes_of((LANES, LANES)).astype(jnp.float32).astype(jnp.bfloat16)
    first_code = (lanes_of((LANES, LANES)) + LANES).astype(jnp.float32).astype(jnp.bfloat16)
    rest_code = (-1 - lanes_of((LANES, LANES))).astype(jnp.float32).astype(jnp.bfloat16)
    one = jnp.ones((LANES, LANES), jnp.bfloat16)
    zero = jnp.zeros((LANES, LANES), jnp.bfloat16)

    def send_of(number, row):
        source = near_ref if number % grid.gz == 0 else far_ref
        return source[number // grid.gz, pl.ds(send_row + row, 1), :]

    for number in range(grid.lists):
        i, j = number // grid.gy, number % grid.gy
        to_x = send_of(grid.domain(i, j, zone_list[0]), 0)
        rest = jnp.zeros((1, LANES), jnp.float32)
        for direction, start, stop in grid.zones:
            row = send_of(grid.domain(i, j, direction), 1)
            rest = jnp.where((lane[:1] >= start) & (lane[:1] < stop), row, rest)
        both = jnp.concatenate([to_x, rest] + [jnp.zeros((6, LANES), jnp.float32)], axis=0)
        index_ref[number] = both.astype(jnp.int32)

    def one_list(number, carry):
        first = near_ref[number, pl.ds(pair_row, blocks), :]
        second = near_ref[number, pl.ds(pair_row + blocks, blocks), :]
        fill = jnp.full((grid.padded - blocks, LANES), float(grid.dummy), jnp.float32)
        parts = [[first, fill], [second, fill]] if grid.padded > blocks else [[first], [second]]
        first, second = (jnp.concatenate(p, axis=0) for p in parts)
        ids_ref[0, number] = first.astype(jnp.int32)
        ids_ref[1, number] = second.astype(jnp.int32)
        usable = jnp.where(first < float(grid.dummy), 1.0, 0.0)
        weight_ref[number] = jnp.where(first == second, 0.5, 1.0) * usable
        both = index_ref[number].astype(jnp.float32)
        codes = jnp.concatenate([first, second], axis=0)
        codes = jnp.where(codes < 2.0 * LANES, codes, 2.0 * LANES - 1.0 - codes)
        turned = jnp.transpose(jnp.concatenate([codes, both], axis=0))
        for side in range(2):
            for block in range(blocks):
                at = side * grid.padded + block
                column = jnp.broadcast_to(turned[:, at : at + 1], (LANES, LANES)).astype(jnp.bfloat16)
                rows = pl.ds((side * blocks + block) * LANES, LANES)
                for part, code in enumerate((own_code, first_code, rest_code)):
                    table_ref[number, rows, pl.ds(part * LANES, LANES)] = jnp.where(column == code, one, zero)
        at = 2 * grid.padded
        column = jnp.broadcast_to(turned[:, at : at + 1], (LANES, LANES)).astype(jnp.bfloat16)
        zone_ref[number, :, pl.ds(0, LANES)] = jnp.where(column == own_code, one, zero)
        column = jnp.broadcast_to(turned[:, at + 1 : at + 2], (LANES, LANES)).astype(jnp.bfloat16)
        slot = lax.broadcasted_iota(jnp.int32, (LANES, LANES), 0).astype(jnp.float32).astype(jnp.bfloat16)
        for part, (direction, start, stop) in enumerate(grid.zones):
            here = (column == own_code) & (slot >= start) & (slot < stop)
            zone_ref[number, :, pl.ds((part + 1) * LANES, LANES)] = jnp.where(here, one, zero)
        return carry

    lax.fori_loop(0, grid.lists, one_list, 0)


def gather_and_push(grid, number, x_ref, ids_ref, weight_ref, index_ref, ext_ref, push_ref, energy_ref):
    i, j = lax.div(number, grid.gy), lax.rem(number, grid.gy)
    lane = lanes_of((8, LANES))
    cell = (CX, CY, CZ)
    to_x = jnp.broadcast_to(index_ref[number, pl.ds(0, 1), :], (8, LANES))
    rest = jnp.broadcast_to(index_ref[number, pl.ds(1, 1), :], (8, LANES))
    for c in range(3):
        ext_ref[c, 0] = x_ref[c, grid.rows_of(i, j, (0, 0, 0)), :]
        shift = float(zone_list[0][c] * cell[c])
        ext_ref[c, 1] = take_lanes(x_ref[c, grid.rows_of(i, j, zone_list[0]), :], to_x) + shift
        value = jnp.zeros((8, LANES), jnp.float32)
        for direction, start, stop in grid.zones:
            shift = float(direction[c] * cell[c])
            got = take_lanes(x_ref[c, grid.rows_of(i, j, direction), :], rest) + shift
            value = jnp.where((lane >= start) & (lane < stop), got, value)
        ext_ref[c, 2] = value
    for group in range(grid.padded // 8):
        sides = []
        for side in range(2):
            ids = ids_ref[side, number, pl.ds(8 * group, 8), :]
            low = ids & (LANES - 1)
            in_own = ids < LANES
            in_first = ids < 2 * LANES
            coords = []
            for c in range(3):
                line = []
                for bead in range(8):
                    a, b, d = (
                        take_lanes(jnp.broadcast_to(ext_ref[c, part, pl.ds(bead, 1), :], (8, LANES)), low)
                        for part in range(3)
                    )
                    line.append(jnp.where(in_own, a, jnp.where(in_first, b, d)))
                coords.append(line)
            sides.append(coords)
        weight = weight_ref[number, pl.ds(8 * group, 8), :]
        scale = weight * (6.0 * strength)
        energy = None
        on_second = [[None] * 8 for _ in range(3)]
        for k in range(8):
            on_first = [None] * 3
            for l in range(8):
                apart = [sides[0][c][k] - sides[1][c][l] for c in range(3)]
                scaled = apart[0] * apart[0] + apart[1] * apart[1] + apart[2] * apart[2]
                intersect = jnp.maximum(1.0 - scaled, 0.0)
                square = intersect * intersect
                cube = square * intersect
                energy = cube if energy is None else energy + cube
                for c in range(3):
                    pushing = square * apart[c]
                    on_first[c] = pushing if l == 0 else on_first[c] + pushing
                    on_second[c][l] = pushing if k == 0 else on_second[c][l] + pushing
            for c in range(3):
                row = (8 * group) * ROWS + c * 8 + k
                push_ref[pl.ds(row, 8, stride=ROWS), :] = on_first[c] * scale
        for c in range(3):
            for l in range(8):
                row = (grid.padded + 8 * group) * ROWS + c * 8 + l
                push_ref[pl.ds(row, 8, stride=ROWS), :] = -(on_second[c][l] * scale)
        own_beads = jnp.where(weight == 0.5, 8.0, 0.0)
        energy_ref[...] += strength * weight * (energy - own_beads)


def scatter(grid, number, push_ref, table_ref, force_ref, halo_ref):
    pieces = []
    for side in range(2):
        for block in range(grid.blocks):
            pieces.append(push_ref[pl.ds((side * grid.padded + block) * ROWS, ROWS), :])
    pushes = split_rows(jnp.concatenate(pieces, axis=1))
    sums = joined(jnp.dot(pushes, table_ref[number], preferred_element_type=jnp.float32))
    row = pl.multiple_of(number * grid.gz * 8, 8)
    for c in range(3):
        force_ref[pl.ds(c * grid.domains * 8 + row, 8), :] = sums[8 * c : 8 * c + 8, :LANES]
    halo_ref[number] = sums[:, LANES:]


def pair_forces(grid, x_ref, tables, force_ref, scratch):
    ids_ref, weight_ref, index_ref, table_ref, zone_ref = tables
    ext_a, ext_b, push_a, push_b, halo_ref, energy_ref = scratch
    force_ref[...] = jnp.zeros(force_ref.shape, jnp.float32)
    energy_ref[...] = jnp.zeros((8, LANES), jnp.float32)

    def forward(number, ext_ref, push_ref):
        gather_and_push(grid, number, x_ref, ids_ref, weight_ref, index_ref, ext_ref, push_ref, energy_ref)

    def back(number, push_ref):
        scatter(grid, number, push_ref, table_ref, force_ref, halo_ref)

    forward(0, ext_a, push_a)

    def two(m, carry):
        back(2 * m, push_a)
        forward(2 * m + 1, ext_b, push_b)
        back(2 * m + 1, push_b)
        forward(2 * m + 2, ext_a, push_a)
        return carry

    lax.fori_loop(0, grid.lists // 2 - 1, two, 0)
    back(grid.lists - 2, push_a)
    forward(grid.lists - 1, ext_b, push_b)
    back(grid.lists - 1, push_b)
    for number in range(grid.lists):
        i, j = number // grid.gy, number % grid.gy
        halo = halo_ref[number]
        to_x = joined(
            jnp.dot(split_rows(halo[:, :LANES]), zone_ref[number, :, pl.ds(0, LANES)], preferred_element_type=jnp.float32)
        )
        rest = joined(
            jnp.dot(
                split_rows(halo[:, LANES:]),
                zone_ref[number, :, pl.ds(LANES, len(grid.zones) * LANES)],
                preferred_element_type=jnp.float32,
            )
        )
        targets = [(zone_list[0], to_x)]
        for part, (direction, start, stop) in enumerate(grid.zones):
            targets.append((direction, rest[:, part * LANES : (part + 1) * LANES]))
        for direction, value in targets:
            row = grid.domain(i, j, direction) * 8
            for c in range(3):
                force_ref[pl.ds(c * grid.domains * 8 + row, 8), :] += value[8 * c : 8 * c + 8]
    force_ref[pl.ds(3 * grid.domains * 8, 8), :] = energy_ref[...]


def start_kernel(grid, layout, near_ref, far_ref, *refs):
    x_ref, v_ref, rest_ref, flag_ref, ids_ref, weight_ref, index_ref, table_ref, zone_ref, force_ref = refs[:10]
    scratch = refs[10:]
    for number in range(grid.domains):
        source = near_ref if number % grid.gz == 0 else far_ref
        at = number // grid.gz
        rows = pl.ds(number * 8, 8)
        for c in range(3):
            x_ref[c, rows, :] = source[at, pl.ds(layout["positions"] + 8 * c, 8), :]
            v_ref[c, rows, :] = source[at, pl.ds(layout["velocities"] + 8 * c, 8), :]
        flag_ref[rows, :] = source[at, pl.ds(layout["flags"], 8), :]
    rest_ref[...] = link_length([x_ref[c] for c in range(3)])
    build_tables(grid, near_ref, far_ref, layout["pairs"], layout["sends"], ids_ref, weight_ref, index_ref, table_ref, zone_ref)
    pair_forces(grid, x_ref, (ids_ref, weight_ref, index_ref, table_ref, zone_ref), force_ref, scratch)


def up(value):
    return pltpu.roll(value, value.shape[0] - 1, 0)


def down(value):
    return pltpu.roll(value, 1, 0)


def dot3(a, b):
    return a[0] * b[0] + a[1] * b[1] + a[2] * b[2]


def links_of(x):
    return [c - up(c) for c in x]


def link_length(x):
    vectors = links_of(x)
    return jnp.sqrt(dot3(vectors, vectors))


def expand_rows(coupling, before, source):
    series = source
    result = source
    for expansion in range(NORDER):
        series = before * down(series) + coupling * up(series)
        result = result + series
    return result


def apply_rows(x, directions, solution):
    moved = []
    for c in range(3):
        shift = directions[c] * (root_half * solution)
        moved.append(x[c] - shift + down(shift))
    return moved


def constrain_rows(previous, updated, rest, flags):
    old = links_of(previous)
    length = jnp.maximum(jnp.sqrt(dot3(old, old)), 0.2)
    directions = [c / length for c in old]
    coupling = 0.5 * dot3(directions, [up(c) for c in directions]) * flags * up(flags)
    before = down(coupling)
    projected = dot3(directions, links_of(updated))
    solution = expand_rows(coupling, before, flags * (root_half * (projected - rest)))
    updated = apply_rows(updated, directions, solution)
    vectors = links_of(updated)
    squared = dot3(vectors, vectors)
    target = jnp.sqrt(jnp.maximum(2.0 * rest * rest - squared, 0.25 * rest * rest))
    solution = expand_rows(coupling, before, flags * (root_half * (rest - target)))
    return apply_rows(updated, directions, solution)


def total_force(grid, own_ref, got_refs):
    size = grid.domains * 8
    total = []
    for c in range(3):
        pieces = []
        for number in range(grid.domains):
            base, k = number // grid.gz * grid.gz, number % grid.gz
            value = own_ref[pl.ds(c * size + number * 8, 8), :]
            for by, ref in enumerate(got_refs, 1):
                value = value + ref[pl.ds(c * size + (base + (k - by) % grid.gz) * 8, 8), :]
            pieces.append(value)
        total.append(jnp.concatenate(pieces, axis=0))
    return total


def energy_row(grid, own_ref, got_refs, v, step, previous):
    rows = pl.ds(3 * grid.domains * 8, 8)
    potential = own_ref[rows, :]
    for ref in got_refs:
        potential = potential + ref[rows, :]
    kinetic = 0.5 * dot3(v, v)
    here = lanes_of((8, LANES)) == step
    row = lax.broadcasted_iota(jnp.int32, (8, LANES), 0)
    previous = jnp.where(here & (row == 0), jnp.sum(potential), previous)
    return jnp.where(here & (row == 1), jnp.sum(kinetic), previous)


def step_kernel(grid, step, x_ref, v_ref, rest_ref, flag_ref, ids_ref, weight_ref, index_ref, table_ref, zone_ref, energies_ref, own_ref, *refs):
    got_refs, refs = refs[: grid.gz - 1], refs[grid.gz - 1 :]
    moved_ref, half_ref, energy_out_ref, force_ref = refs[:4]
    scratch = refs[4:]
    force = total_force(grid, own_ref, got_refs)
    x = [x_ref[c] for c in range(3)]
    v = [v_ref[c] for c in range(3)]
    if step > 0:
        v = [v[c] + (0.5 * time_step) * force[c] for c in range(3)]
        energy_out_ref[...] = energy_row(grid, own_ref, got_refs, v, step - 1, energies_ref[...])
    else:
        energy_out_ref[...] = energies_ref[...]
    half = [v[c] + (0.5 * time_step) * force[c] for c in range(3)]
    moved = constrain_rows(x, [x[c] + time_step * half[c] for c in range(3)], rest_ref[...], flag_ref[...])
    for c in range(3):
        moved_ref[c] = moved[c]
        half_ref[c] = (moved[c] - x[c]) / time_step
    pair_forces(grid, moved_ref, (ids_ref, weight_ref, index_ref, table_ref, zone_ref), force_ref, scratch)


def last_kernel(grid, bead_total, x_ref, v_ref, energies_ref, own_ref, *refs):
    got_refs, refs = refs[: grid.gz - 1], refs[grid.gz - 1 :]
    targets, (place_ref, speed_ref, energy_out_ref), sems = refs[:3], refs[3:6], refs[6]
    force = total_force(grid, own_ref, got_refs)
    v = [v_ref[c] + (0.5 * time_step) * force[c] for c in range(3)]
    for c in range(3):
        place_ref[c] = x_ref[c, pl.ds(0, 8), :]
        speed_ref[c] = v[c][:8]
    energies = energy_row(grid, own_ref, got_refs, v, ITERS - 1, energies_ref[...])
    energy_out_ref[...] = energies[:2, :ITERS] / bead_total
    moved_together((place_ref, speed_ref, energy_out_ref), targets, sems)


def moved_together(sources, targets, sems):
    copies = [pltpu.make_async_copy(a, b, sems.at[n]) for n, (a, b) in enumerate(zip(sources, targets))]
    for copy in copies:
        copy.start()
    for copy in copies:
        copy.wait()


def pack_kernel(grid, layout, *refs):
    sources, out_ref, held, sems = refs[:5], refs[5], refs[6:11], refs[11]
    moved_together(sources, held, sems)
    x_ref, v_ref, flag_ref, pair_ref, send_ref = held
    out_ref[...] = jnp.zeros(out_ref.shape, jnp.float32)
    for c in range(3):
        out_ref[pl.ds(layout["positions"] + 8 * c, 8), :] = x_ref[c]
        out_ref[pl.ds(layout["velocities"] + 8 * c, 8), :] = v_ref[c]
    out_ref[pl.ds(layout["flags"], 7), :] = flag_ref[...].astype(jnp.float32)
    for side in range(2):
        for block in range(grid.blocks):
            row = layout["pairs"] + side * grid.blocks + block
            ids = pair_ref[pl.ds(side, 1), pl.ds(block * LANES, LANES)]
            out_ref[pl.ds(row, 1), :] = ids.astype(jnp.float32)
    out_ref[pl.ds(layout["sends"], 1), :] = send_ref[:, :LANES].astype(jnp.float32)
    rest = send_ref.shape[1] - LANES
    out_ref[pl.ds(layout["sends"] + 1, 1), pl.ds(0, rest)] = send_ref[:, LANES:].astype(jnp.float32)


def from_ahead(value, steps):
    names = [a for a, by in zip(("gx", "gy", "gz"), steps) if by]
    if not names:
        return value
    counts = [lax.axis_size(a) for a in names]
    pairs = []
    for target in np.ndindex(*counts):
        source = [(t + by) % n for t, by, n in zip(target, [s for s in steps if s], counts)]
        pairs.append(tuple(int(np.ravel_multi_index(p, counts)) for p in (source, target)))
    return lax.ppermute(value, tuple(names), pairs)


def replicated(grid, positions, velocities, send_list, pair_list, constraint_flags):
    clusters = positions.shape[2]
    heights = dict(positions=ROWS, velocities=ROWS, flags=8, pairs=2 * grid.blocks, sends=2)
    layout, row = {}, 0
    for name, height in heights.items():
        layout[name] = row
        row += height
    params = pltpu.CompilerParams(vmem_limit_bytes=VMEM_LIMIT)

    def call(kernel, shapes, scratch, *values, **specs):
        return pl.pallas_call(kernel, out_shape=shapes, scratch_shapes=scratch, compiler_params=params, **specs)(*values)

    anywhere = pl.BlockSpec(memory_space=pltpu.MemorySpace.HBM)
    given = (positions, velocities, constraint_flags, pair_list, send_list.reshape(1, -1))
    given = [pltpu.with_memory_space_constraint(value, pltpu.MemorySpace.HBM) for value in given]

    pack = call(
        functools.partial(pack_kernel, grid, layout),
        jax.ShapeDtypeStruct((row + -row % 8, LANES), jnp.float32),
        [pltpu.VMEM(value.shape, value.dtype) for value in given] + [pltpu.SemaphoreType.DMA((len(given),))],
        *given,
        in_specs=[anywhere] * len(given),
    )
    column = jnp.stack([from_ahead(pack, (0, j, 0)) for j in range(grid.gy)])
    near = jnp.concatenate([from_ahead(column, (i, 0, 0)) for i in range(grid.gx)], axis=0)
    far = from_ahead(near, (0, 0, 1))
    f32, i32, b16 = jnp.float32, jnp.int32, jnp.bfloat16
    n, rows = grid.lists, grid.domains * 8
    cube = jax.ShapeDtypeStruct((3, rows, LANES), f32)
    plane = jax.ShapeDtypeStruct((rows, LANES), f32)
    small = jax.ShapeDtypeStruct((8, LANES), f32)
    forces = jax.ShapeDtypeStruct((3 * rows + 8, LANES), f32)
    table_shapes = [
        jax.ShapeDtypeStruct((2, n, grid.padded, LANES), i32),
        jax.ShapeDtypeStruct((n, grid.padded, LANES), f32),
        jax.ShapeDtypeStruct((n, 8, LANES), i32),
        jax.ShapeDtypeStruct((n, grid.slots, 3 * LANES), b16),
        jax.ShapeDtypeStruct((n, LANES, len(zone_list) * LANES), b16),
    ]
    scratch = [
        pltpu.VMEM((3, 3, 8, LANES), f32),
        pltpu.VMEM((3, 3, 8, LANES), f32),
        pltpu.VMEM((2 * grid.padded * ROWS, LANES), f32),
        pltpu.VMEM((2 * grid.padded * ROWS, LANES), f32),
        pltpu.VMEM((n, ROWS, 2 * LANES), f32),
        pltpu.VMEM((8, LANES), f32),
    ]
    x, v, rest, flags, *rest_out = call(
        functools.partial(start_kernel, grid, layout), [cube, cube, plane, plane] + table_shapes + [forces], scratch, near, far
    )
    tables, force = rest_out[:5], rest_out[5]
    energies = jnp.zeros((8, LANES), f32)
    for step in range(ITERS):
        got = [from_ahead(force, (0, 0, by)) for by in range(1, grid.gz)]
        x, v, energies, force = call(
            functools.partial(step_kernel, grid, step),
            [cube, cube, small, forces],
            scratch,
            x, v, rest, flags, *tables, energies, force, *got,
        )
    got = [from_ahead(force, (0, 0, by)) for by in range(1, grid.gz)]
    own = jax.ShapeDtypeStruct((3, 8, LANES), f32)
    shapes = [own, own, jax.ShapeDtypeStruct((2, ITERS), f32)]
    place, speed, energies = call(
        functools.partial(last_kernel, grid, 8 * clusters * grid.domains),
        shapes,
        [pltpu.VMEM(shape.shape, f32) for shape in shapes] + [pltpu.SemaphoreType.DMA((len(shapes),))],
        x, v, energies, force, *got,
        out_specs=[anywhere] * len(shapes),
    )
    return (place, speed, energies.T)


def can_replicate(grid, positions, send_list, pair_list):
    return (
        grid.domains <= MAX_REPLICATED
        and grid.lists % 2 == 0
        and grid.gz == 2
        and positions.shape[2] == LANES
        and zone_sizes()[0] == LANES
        and pair_list.shape[1] % LANES == 0
        and sum(zone_sizes()) == send_list.shape[0]
        and send_list.shape[0] - LANES < LANES
    )


VMEM_LIMIT = 16 * 1024 * 1024


def solution(mesh):
    def on_any(positions, velocities, send_list, pair_list, constraint_flags):
        grid = Grid(mesh, pair_list.shape[1], send_list.shape[0])
        if can_replicate(grid, positions, send_list, pair_list):
            return replicated(grid, positions, velocities, send_list, pair_list, constraint_flags)
        return on_device(positions, velocities, send_list, pair_list, constraint_flags)

    return jax.shard_map(
        on_any,
        mesh=mesh,
        in_specs=(
            P(None, None, ("runs", "gx", "gy", "gz")),
            P(None, None, ("runs", "gx", "gy", "gz")),
            P(("runs", "gx", "gy", "gz")),
            P(None, ("runs", "gx", "gy", "gz")),
            P(None, ("runs", "gx", "gy", "gz")),
        ),
        out_specs=(
            P(None, None, ("runs", "gx", "gy", "gz")),
            P(None, None, ("runs", "gx", "gy", "gz")),
            P("runs", None),
        ),
        check_vma=False,
    )
```

```python
import functools

import jax
import jax.numpy as jnp
import numpy as np
from jax import lax
from jax.experimental import pallas as pl
from jax.experimental.pallas import tpu as pltpu
from jax.sharding import PartitionSpec as P

CX = 1
CY = 8
CZ = 16
ITERS = 3
NORDER = 4


time_step = 0.02
strength = 2.0
root_half = 0.7071067811865476
zone_list = ((1, 0, 0), (0, 1, 0), (0, 0, 1), (1, 1, 0), (1, 0, 1), (0, 1, 1), (1, 1, 1))


def from_behind(value, axis, by):
    count = lax.axis_size(axis)
    return lax.ppermute(value, axis, [(i, (i + by) % count) for i in range(count)])


def zone_sizes():
    return tuple(
        (
            (CX if direction[0] == 0 else 1)
            * (CY if direction[1] == 0 else 1)
            * (CZ if direction[2] == 0 else 1)
            for direction in zone_list
        )
    )


def split_blocks(packed, block_sizes):
    pieces = []
    position = 0
    for length in block_sizes:
        pieces.append(packed[:, :, position : position + length])
        position += length
    return pieces


def shell_offsets():
    block_sizes = zone_sizes()
    columns = []
    for number in range(7):
        direction = zone_list[number]
        column = np.array(
            [[direction[0] * CX], [direction[1] * CY], [direction[2] * CZ]], np.float32
        )
        columns.append(np.tile(column, (1, block_sizes[number])))
    return jnp.asarray(np.concatenate(columns, axis=1))[:, None, :]


def share_coords(coords, send_table):
    sizes_all = zone_sizes()
    chosen = jnp.dot(
        coords.reshape(24, -1), send_table, precision=lax.Precision.HIGHEST
    ).reshape(3, 8, -1)
    outgoing = split_blocks(chosen, sizes_all)
    along_y = from_behind(
        jnp.concatenate([outgoing[1], outgoing[3], outgoing[5], outgoing[6]], axis=2), "gy", -1
    )
    got_y = split_blocks(along_y, [sizes_all[1], sizes_all[3], sizes_all[5], sizes_all[6]])
    along_x = from_behind(
        jnp.concatenate([outgoing[0], outgoing[4], got_y[1], got_y[3]], axis=2), "gx", -1
    )
    got_x = split_blocks(along_x, [sizes_all[0], sizes_all[4], sizes_all[3], sizes_all[6]])
    along_z = from_behind(
        jnp.concatenate([outgoing[2], got_x[1], got_y[2], got_x[3]], axis=2), "gz", -1
    )
    got_z = split_blocks(along_z, [sizes_all[2], sizes_all[4], sizes_all[5], sizes_all[6]])
    received = [got_x[0], got_y[0], got_z[0], got_x[2], got_z[1], got_z[2], got_z[3]]
    return jnp.concatenate(received, axis=2) + shell_offsets()


def return_forces(halo_forces):
    sizes_all = zone_sizes()
    outgoing = split_blocks(halo_forces, sizes_all)
    along_z = from_behind(
        jnp.concatenate([outgoing[2], outgoing[4], outgoing[5], outgoing[6]], axis=2), "gz", 1
    )
    got_z = split_blocks(along_z, [sizes_all[2], sizes_all[4], sizes_all[5], sizes_all[6]])
    along_x = from_behind(
        jnp.concatenate([outgoing[0], outgoing[3], got_z[1], got_z[3]], axis=2), "gx", 1
    )
    got_x = split_blocks(along_x, [sizes_all[0], sizes_all[3], sizes_all[4], sizes_all[6]])
    settled = [got_x[0], got_z[0], got_x[2]]
    pending = [got_x[1], got_z[2], got_x[3]]
    along_y = from_behind(
        jnp.concatenate([outgoing[1], pending[0], pending[1], pending[2]], axis=2), "gy", 1
    )
    got_y = split_blocks(along_y, [sizes_all[1], sizes_all[3], sizes_all[5], sizes_all[6]])
    return jnp.concatenate(
        [settled[0], got_y[0], settled[1], got_y[1], settled[2], got_y[2], got_y[3]], axis=2
    )


def pair_tables(pair_list, extended_count):
    rows = lax.broadcasted_iota(jnp.int32, (extended_count, pair_list.shape[1]), 0)
    first_table = (rows == pair_list[0][None, :]).astype(jnp.float32)
    second_table = (rows == pair_list[1][None, :]).astype(jnp.float32)
    return (first_table, second_table)


def domain_forces(extended, pair_list, tables):
    extended_count = extended.shape[2]
    slot_count = pair_list.shape[1]
    first_ids = pair_list[0]
    second_ids = pair_list[1]
    flat = extended.reshape(24, extended_count)
    first_coords = jnp.dot(flat, tables[0], precision=lax.Precision.HIGHEST).reshape(
        3, 8, slot_count
    )
    second_coords = jnp.dot(flat, tables[1], precision=lax.Precision.HIGHEST).reshape(
        3, 8, slot_count
    )
    separation = first_coords[:, :, None, :] - second_coords[:, None, :, :]
    scaled = jnp.sum(separation * separation, axis=0)
    intersect = jnp.maximum(1.0 - scaled, 0.0)
    bead_row = lax.broadcasted_iota(jnp.int32, (8, 8, 1), 0)
    bead_column = lax.broadcasted_iota(jnp.int32, (8, 8, 1), 1)
    self_pair = (first_ids == second_ids)[None, None, :]
    usable = (first_ids < extended_count - 1)[None, None, :]
    weight = (jnp.where(self_pair, bead_row < bead_column, True) & usable).astype(jnp.float32)
    energy = strength * jnp.sum(weight * intersect * intersect * intersect)
    magnitude = 6.0 * strength * weight * intersect * intersect
    pushing = magnitude[None] * separation
    on_first = jnp.sum(pushing, axis=2).reshape(24, slot_count)
    on_second = (-jnp.sum(pushing, axis=1)).reshape(24, slot_count)
    contract = (((1,), (1,)), ((), ()))
    forces = lax.dot_general(on_first, tables[0], contract, precision=lax.Precision.HIGHEST)
    forces = forces + lax.dot_general(
        on_second, tables[1], contract, precision=lax.Precision.HIGHEST
    )
    return (forces.reshape(3, 8, extended_count), energy)


def local_forces(coords, send_table, pair_list, tables):
    halo_coords = share_coords(coords, send_table)
    dummy_cluster = jnp.zeros((3, 8, 1), jnp.float32)
    extended = jnp.concatenate([coords, halo_coords, dummy_cluster], axis=2)
    forces, energy = domain_forces(extended, pair_list, tables)
    cluster_count = coords.shape[2]
    returned = return_forces(forces[:, :, cluster_count : cluster_count + send_table.shape[1]])
    contract = (((1,), (1,)), ((), ()))
    added = lax.dot_general(
        returned.reshape(24, -1), send_table, contract, precision=lax.Precision.HIGHEST
    )
    home_forces = forces[:, :, :cluster_count] + added.reshape(3, 8, -1)
    return (home_forces, energy)


def link_vectors(coords):
    return coords[:, :-1, :] - coords[:, 1:, :]


def link_lengths(coords):
    vectors = link_vectors(coords)
    return jnp.sqrt(jnp.sum(vectors * vectors, axis=0))


def expand(coupling, source):
    coupling_down = jnp.pad(coupling, ((1, 0), (0, 0)))
    coupling_up = jnp.pad(coupling, ((0, 1), (0, 0)))
    series = source
    result = source
    for expansion in range(NORDER):
        series = (
            coupling_down * jnp.pad(series, ((1, 0), (0, 0)))[:-1]
            + coupling_up * jnp.pad(series, ((0, 1), (0, 0)))[1:]
        )
        result = result + series
    return result


def apply_links(coords, directions, solution):
    shifts = directions * (root_half * solution)[None]
    return (
        coords
        - jnp.pad(shifts, ((0, 0), (0, 1), (0, 0)))
        + jnp.pad(shifts, ((0, 0), (1, 0), (0, 0)))
    )


def constrain(previous, updated, rest_length, link_flags):
    old_vectors = link_vectors(previous)
    directions = (
        old_vectors / jnp.maximum(jnp.sqrt(jnp.sum(old_vectors * old_vectors, axis=0)), 0.2)[None]
    )
    coupling = (
        0.5
        * jnp.sum(directions[:, :-1] * directions[:, 1:], axis=0)
        * link_flags[:-1]
        * link_flags[1:]
    )
    projected = jnp.sum(directions * link_vectors(updated), axis=0)
    solution = expand(coupling, link_flags * root_half * (projected - rest_length))
    updated = apply_links(updated, directions, solution)
    vectors = link_vectors(updated)
    squared = jnp.sum(vectors * vectors, axis=0)
    target = jnp.sqrt(
        jnp.maximum(2.0 * rest_length * rest_length - squared, 0.25 * rest_length * rest_length)
    )
    solution = expand(coupling, link_flags * root_half * (rest_length - target))
    updated = apply_links(updated, directions, solution)
    return updated


def total_over(value, axis):
    count = lax.axis_size(axis)
    if count > 4:
        return lax.psum(value, axis)
    total = value
    for by in range(1, count):
        total = total + from_behind(value, axis, by)
    return total


def on_device(positions, velocities, send_list, pair_list, constraint_flags):
    link_flags = constraint_flags.astype(jnp.float32)
    rest_length = link_lengths(positions)
    bead_total = 8 * positions.shape[2] * lax.axis_size(("gx", "gy", "gz"))
    tables = pair_tables(pair_list, positions.shape[2] + send_list.shape[0] + 1)
    owned = lax.broadcasted_iota(jnp.int32, (positions.shape[2], send_list.shape[0]), 0)
    send_table = (owned == send_list[None, :]).astype(jnp.float32)
    forces, potential = local_forces(positions, send_table, pair_list, tables)
    energy_rows = []
    for iteration in range(ITERS):
        half_speed = velocities + 0.5 * time_step * forces
        updated = constrain(positions, positions + time_step * half_speed, rest_length, link_flags)
        half_speed = (updated - positions) / time_step
        forces, potential = local_forces(updated, send_table, pair_list, tables)
        velocities = half_speed + 0.5 * time_step * forces
        positions = updated
        kinetic = 0.5 * jnp.sum(velocities * velocities)
        energy_rows.append(jnp.stack([potential, kinetic]))
    energies = jnp.stack(energy_rows)
    for axis in ("gz", "gy", "gx"):
        energies = total_over(energies, axis)
    return (positions, velocities, energies / bead_total)


LANES = 128
ROWS = 24
MAX_REPLICATED = 16


def split_rows(value):
    high = value.astype(jnp.bfloat16).astype(jnp.float32)
    return jnp.concatenate([high, value - high], axis=0).astype(jnp.bfloat16)


def joined(value):
    return value[:ROWS] + value[ROWS:]


class Grid:
    def __init__(self, mesh, slot_count, halo_count):
        self.gx, self.gy, self.gz = (mesh.shape[a] for a in ("gx", "gy", "gz"))
        self.domains = self.gx * self.gy * self.gz
        self.lists = self.gx * self.gy
        self.blocks = slot_count // LANES
        self.padded = (self.blocks + 7) // 8 * 8
        self.dummy = LANES + halo_count
        self.slots = 2 * self.blocks * LANES
        sizes = zone_sizes()
        self.zones = []
        start = 0
        for direction, size in zip(zone_list[1:], sizes[1:]):
            self.zones.append((direction, start, start + size))
            start += size

    def domain(self, i, j, direction):
        i = lax.rem(i + direction[0], self.gx) if not isinstance(i, int) else (i + direction[0]) % self.gx
        j = lax.rem(j + direction[1], self.gy) if not isinstance(j, int) else (j + direction[1]) % self.gy
        return (i * self.gy + j) * self.gz + direction[2] % self.gz

    def rows_of(self, i, j, direction):
        row = self.domain(i, j, direction) * 8
        return pl.ds(row if isinstance(row, int) else pl.multiple_of(row, 8), 8)


def lanes_of(shape):
    return lax.broadcasted_iota(jnp.int32, shape, 1)


def take_lanes(source, index):
    return jnp.take_along_axis(source, index, axis=1, mode="promise_in_bounds")


def rounded_iota(shape, dimension, start=0):
    return (lax.broadcasted_iota(jnp.int32, shape, dimension) + start).astype(jnp.float32).astype(jnp.bfloat16)


def table_kernel(grid, pair_row, near_ref, ids_ref, weight_ref, table_ref, spread_ref, turned_ref):
    blocks = grid.blocks
    square = (LANES, LANES)
    codes_of = (rounded_iota(square, 1), rounded_iota(square, 1, LANES), -rounded_iota(square, 1, 1))
    one, zero = jnp.ones(square, jnp.bfloat16), jnp.zeros(square, jnp.bfloat16)
    row = rounded_iota(square, 0)
    for at in range(2 * blocks):
        place = at // blocks * grid.padded + at % blocks
        spread_ref[:, pl.ds(at * LANES, LANES)] = jnp.where(row == place, one, zero)
    for number in range(grid.lists):
        sides = []
        for side in range(2):
            ids = near_ref[number, pl.ds(pair_row + side * blocks, blocks), :]
            fill = jnp.full((grid.padded - blocks, LANES), float(grid.dummy), jnp.float32)
            sides.append(jnp.concatenate([ids, fill], axis=0) if grid.padded > blocks else ids)
            ids_ref[side, number] = sides[side].astype(jnp.int32)
        usable = jnp.where(sides[0] < float(grid.dummy), 1.0, 0.0)
        weight_ref[number] = jnp.where(sides[0] == sides[1], 0.5, 1.0) * usable
        codes = jnp.concatenate(sides, axis=0)
        codes = jnp.where(codes < 2.0 * LANES, codes, 2.0 * LANES - 1.0 - codes)
        empty = jnp.zeros((LANES - 2 * grid.padded, LANES), jnp.float32)
        turned_ref[number] = jnp.transpose(jnp.concatenate([codes, empty], axis=0)).astype(jnp.bfloat16)

    def one_list(number, carry):
        wide = jnp.dot(turned_ref[number], spread_ref[...], preferred_element_type=jnp.float32)
        for at in range(2 * blocks):
            column = wide[:, at * LANES : (at + 1) * LANES].astype(jnp.bfloat16)
            for part, code in enumerate(codes_of):
                hot = jnp.where(column == code, one, zero)
                table_ref[number, part, pl.ds(at * LANES, LANES), :] = hot
        return carry

    lax.fori_loop(0, grid.lists, one_list, 0)


def build_zones(grid, near_ref, far_ref, send_row, index_ref, zone_ref):
    square = (LANES, LANES)
    lane = lanes_of((1, LANES))
    own_code = rounded_iota(square, 1)
    slot = rounded_iota(square, 0)
    one, zero = jnp.ones(square, jnp.bfloat16), jnp.zeros(square, jnp.bfloat16)

    def send_of(number, row):
        source = near_ref if number % grid.gz == 0 else far_ref
        return source[number // grid.gz, pl.ds(send_row + row, 1), :]

    for number in range(grid.lists):
        i, j = number // grid.gy, number % grid.gy
        to_x = send_of(grid.domain(i, j, zone_list[0]), 0)
        rest = jnp.zeros((1, LANES), jnp.float32)
        for direction, start, stop in grid.zones:
            row = send_of(grid.domain(i, j, direction), 1)
            rest = jnp.where((lane >= start) & (lane < stop), row, rest)
        both = jnp.concatenate([to_x, rest] + [jnp.zeros((6, LANES), jnp.float32)], axis=0)
        index_ref[number] = both.astype(jnp.int32)

    def one_list(number, carry):
        turned = jnp.transpose(index_ref[number].astype(jnp.float32))
        column = jnp.broadcast_to(turned[:, 0:1], square).astype(jnp.bfloat16)
        zone_ref[number, 0] = jnp.where(column == own_code, one, zero)
        column = jnp.broadcast_to(turned[:, 1:2], square).astype(jnp.bfloat16)
        for part, (direction, start, stop) in enumerate(grid.zones):
            here = (column == own_code) & (slot >= start) & (slot < stop)
            zone_ref[number, part + 1] = jnp.where(here, one, zero)
        return carry

    lax.fori_loop(0, grid.lists, one_list, 0)


def gather_and_push(grid, number, x_ref, ids_ref, weight_ref, index_ref, ext_ref, push_ref, energy_ref):
    i, j = lax.div(number, grid.gy), lax.rem(number, grid.gy)
    lane = lanes_of((8, LANES))
    cell = (CX, CY, CZ)
    to_x = jnp.broadcast_to(index_ref[number, pl.ds(0, 1), :], (8, LANES))
    rest = jnp.broadcast_to(index_ref[number, pl.ds(1, 1), :], (8, LANES))
    for c in range(3):
        ext_ref[c, 0] = x_ref[c, grid.rows_of(i, j, (0, 0, 0)), :]
        shift = float(zone_list[0][c] * cell[c])
        ext_ref[c, 1] = take_lanes(x_ref[c, grid.rows_of(i, j, zone_list[0]), :], to_x) + shift
        value = jnp.zeros((8, LANES), jnp.float32)
        for direction, start, stop in grid.zones:
            shift = float(direction[c] * cell[c])
            got = take_lanes(x_ref[c, grid.rows_of(i, j, direction), :], rest) + shift
            value = jnp.where((lane >= start) & (lane < stop), got, value)
        ext_ref[c, 2] = value
    for group in range(grid.padded // 8):
        sides = []
        for side in range(2):
            ids = ids_ref[side, number, pl.ds(8 * group, 8), :]
            low = ids & (LANES - 1)
            in_own = ids < LANES
            in_first = ids < 2 * LANES
            coords = []
            for c in range(3):
                line = []
                for bead in range(8):
                    a, b, d = (
                        take_lanes(jnp.broadcast_to(ext_ref[c, part, pl.ds(bead, 1), :], (8, LANES)), low)
                        for part in range(3)
                    )
                    line.append(jnp.where(in_own, a, jnp.where(in_first, b, d)))
                coords.append(line)
            sides.append(coords)
        weight = weight_ref[number, pl.ds(8 * group, 8), :]
        scale = weight * (6.0 * strength)
        energy = None
        partial = [None] * 8
        for half in range(2):
            beads = range(4 * half, 4 * half + 4)
            second = {l: [sides[1][c][l] for c in range(3)] for l in beads}
            on_second = {l: None for l in beads}
            for k in range(8):
                on_first = partial[k]
                first = [sides[0][c][k] for c in range(3)]
                for l in beads:
                    apart = [first[c] - second[l][c] for c in range(3)]
                    scaled = apart[0] * apart[0] + apart[1] * apart[1] + apart[2] * apart[2]
                    intersect = jnp.maximum(1.0 - scaled, 0.0)
                    square = intersect * intersect
                    cube = square * intersect
                    energy = cube if energy is None else energy + cube
                    pushing = [square * apart[c] for c in range(3)]
                    on_first = pushing if on_first is None else [on_first[c] + pushing[c] for c in range(3)]
                    on_second[l] = pushing if k == 0 else [on_second[l][c] + pushing[c] for c in range(3)]
                partial[k] = on_first
                if half == 1:
                    for c in range(3):
                        row = (8 * group) * ROWS + c * 8 + k
                        push_ref[pl.ds(row, 8, stride=ROWS), :] = on_first[c] * scale
            for c in range(3):
                for l in beads:
                    row = (grid.padded + 8 * group) * ROWS + c * 8 + l
                    push_ref[pl.ds(row, 8, stride=ROWS), :] = on_second[l][c] * (-scale)
        own_beads = jnp.where(weight == 0.5, 8.0, 0.0)
        energy_ref[...] += strength * weight * (energy - own_beads)


def scatter(grid, number, push_ref, table_ref, force_ref, halo_ref):
    pieces = []
    for side in range(2):
        for block in range(grid.blocks):
            pieces.append(push_ref[pl.ds((side * grid.padded + block) * ROWS, ROWS), :])
    pushes = split_rows(jnp.concatenate(pieces, axis=1))
    table = jnp.concatenate([table_ref[number, part] for part in range(3)], axis=1)
    sums = joined(jnp.dot(pushes, table, preferred_element_type=jnp.float32))
    row = pl.multiple_of(number * grid.gz * 8, 8)
    for c in range(3):
        force_ref[pl.ds(c * grid.domains * 8 + row, 8), :] = sums[8 * c : 8 * c + 8, :LANES]
    halo_ref[number] = sums[:, LANES:]


def pair_forces(grid, x_ref, tables, force_ref, scratch):
    ids_ref, weight_ref, index_ref, table_ref, zone_ref = tables
    ext_a, ext_b, push_a, push_b, halo_ref, energy_ref = scratch
    force_ref[...] = jnp.zeros(force_ref.shape, jnp.float32)
    energy_ref[...] = jnp.zeros((8, LANES), jnp.float32)

    def forward(number, ext_ref, push_ref):
        gather_and_push(grid, number, x_ref, ids_ref, weight_ref, index_ref, ext_ref, push_ref, energy_ref)

    def back(number, push_ref):
        scatter(grid, number, push_ref, table_ref, force_ref, halo_ref)

    forward(0, ext_a, push_a)

    def two(m, carry):
        back(2 * m, push_a)
        forward(2 * m + 1, ext_b, push_b)
        back(2 * m + 1, push_b)
        forward(2 * m + 2, ext_a, push_a)
        return carry

    lax.fori_loop(0, grid.lists // 2 - 1, two, 0)
    back(grid.lists - 2, push_a)
    forward(grid.lists - 1, ext_b, push_b)
    back(grid.lists - 1, push_b)
    for number in range(grid.lists):
        i, j = number // grid.gy, number % grid.gy
        halo = halo_ref[number]
        to_x = joined(
            jnp.dot(split_rows(halo[:, :LANES]), zone_ref[number, 0], preferred_element_type=jnp.float32)
        )
        rest = joined(
            jnp.dot(
                split_rows(halo[:, LANES:]),
                jnp.concatenate([zone_ref[number, part + 1] for part in range(len(grid.zones))], axis=1),
                preferred_element_type=jnp.float32,
            )
        )
        targets = [(zone_list[0], to_x)]
        for part, (direction, start, stop) in enumerate(grid.zones):
            targets.append((direction, rest[:, part * LANES : (part + 1) * LANES]))
        for direction, value in targets:
            row = grid.domain(i, j, direction) * 8
            for c in range(3):
                force_ref[pl.ds(c * grid.domains * 8 + row, 8), :] += value[8 * c : 8 * c + 8]
    force_ref[pl.ds(3 * grid.domains * 8, 8), :] = energy_ref[...]


def start_kernel(grid, layout, near_ref, far_ref, ids_ref, weight_ref, table_ref, *refs):
    x_ref, v_ref, rest_ref, flag_ref, index_ref, zone_ref, force_ref = refs[:7]
    scratch = refs[7:]
    for number in range(grid.domains):
        source = near_ref if number % grid.gz == 0 else far_ref
        at = number // grid.gz
        rows = pl.ds(number * 8, 8)
        for c in range(3):
            x_ref[c, rows, :] = source[at, pl.ds(layout["positions"] + 8 * c, 8), :]
            v_ref[c, rows, :] = source[at, pl.ds(layout["velocities"] + 8 * c, 8), :]
        flag_ref[rows, :] = source[at, pl.ds(layout["flags"], 8), :]
    rest_ref[...] = link_length([x_ref[c] for c in range(3)])
    build_zones(grid, near_ref, far_ref, layout["sends"], index_ref, zone_ref)
    pair_forces(grid, x_ref, (ids_ref, weight_ref, index_ref, table_ref, zone_ref), force_ref, scratch)


def up(value):
    return pltpu.roll(value, value.shape[0] - 1, 0)


def down(value):
    return pltpu.roll(value, 1, 0)


def dot3(a, b):
    return a[0] * b[0] + a[1] * b[1] + a[2] * b[2]


def links_of(x):
    return [c - up(c) for c in x]


def link_length(x):
    vectors = links_of(x)
    return jnp.sqrt(dot3(vectors, vectors))


def expand_rows(coupling, before, source):
    series = source
    result = source
    for expansion in range(NORDER):
        series = before * down(series) + coupling * up(series)
        result = result + series
    return result


def apply_rows(x, directions, solution):
    moved = []
    for c in range(3):
        shift = directions[c] * (root_half * solution)
        moved.append(x[c] - shift + down(shift))
    return moved


def constrain_rows(previous, updated, rest, flags):
    old = links_of(previous)
    length = jnp.maximum(jnp.sqrt(dot3(old, old)), 0.2)
    directions = [c / length for c in old]
    coupling = 0.5 * dot3(directions, [up(c) for c in directions]) * flags * up(flags)
    before = down(coupling)
    projected = dot3(directions, links_of(updated))
    solution = expand_rows(coupling, before, flags * (root_half * (projected - rest)))
    updated = apply_rows(updated, directions, solution)
    vectors = links_of(updated)
    squared = dot3(vectors, vectors)
    target = jnp.sqrt(jnp.maximum(2.0 * rest * rest - squared, 0.25 * rest * rest))
    solution = expand_rows(coupling, before, flags * (root_half * (rest - target)))
    return apply_rows(updated, directions, solution)


def total_force(grid, own_ref, got_refs):
    size = grid.domains * 8
    total = []
    for c in range(3):
        pieces = []
        for number in range(grid.domains):
            base, k = number // grid.gz * grid.gz, number % grid.gz
            value = own_ref[pl.ds(c * size + number * 8, 8), :]
            for by, ref in enumerate(got_refs, 1):
                value = value + ref[pl.ds(c * size + (base + (k - by) % grid.gz) * 8, 8), :]
            pieces.append(value)
        total.append(jnp.concatenate(pieces, axis=0))
    return total


def energy_row(grid, own_ref, got_refs, v, step, previous):
    rows = pl.ds(3 * grid.domains * 8, 8)
    potential = own_ref[rows, :]
    for ref in got_refs:
        potential = potential + ref[rows, :]
    kinetic = 0.5 * dot3(v, v)
    here = lanes_of((8, LANES)) == step
    row = lax.broadcasted_iota(jnp.int32, (8, LANES), 0)
    previous = jnp.where(here & (row == 0), jnp.sum(potential), previous)
    return jnp.where(here & (row == 1), jnp.sum(kinetic), previous)


def step_kernel(grid, step, x_ref, v_ref, rest_ref, flag_ref, ids_ref, weight_ref, index_ref, table_ref, zone_ref, energies_ref, own_ref, *refs):
    got_refs, refs = refs[: grid.gz - 1], refs[grid.gz - 1 :]
    moved_ref, half_ref, energy_out_ref, force_ref = refs[:4]
    scratch = refs[4:]
    force = total_force(grid, own_ref, got_refs)
    x = [x_ref[c] for c in range(3)]
    v = [v_ref[c] for c in range(3)]
    if step > 0:
        v = [v[c] + (0.5 * time_step) * force[c] for c in range(3)]
        energy_out_ref[...] = energy_row(grid, own_ref, got_refs, v, step - 1, energies_ref[...])
    else:
        energy_out_ref[...] = energies_ref[...]
    half = [v[c] + (0.5 * time_step) * force[c] for c in range(3)]
    moved = constrain_rows(x, [x[c] + time_step * half[c] for c in range(3)], rest_ref[...], flag_ref[...])
    for c in range(3):
        moved_ref[c] = moved[c]
        half_ref[c] = (moved[c] - x[c]) / time_step
    pair_forces(grid, moved_ref, (ids_ref, weight_ref, index_ref, table_ref, zone_ref), force_ref, scratch)


def last_kernel(grid, bead_total, x_ref, v_ref, energies_ref, own_ref, *refs):
    got_refs, refs = refs[: grid.gz - 1], refs[grid.gz - 1 :]
    targets, (place_ref, speed_ref, energy_out_ref), sems = refs[:3], refs[3:6], refs[6]
    force = total_force(grid, own_ref, got_refs)
    v = [v_ref[c] + (0.5 * time_step) * force[c] for c in range(3)]
    for c in range(3):
        place_ref[c] = x_ref[c, pl.ds(0, 8), :]
        speed_ref[c] = v[c][:8]
    energies = energy_row(grid, own_ref, got_refs, v, ITERS - 1, energies_ref[...])
    energy_out_ref[...] = energies[:2, :ITERS] / bead_total
    moved_together((place_ref, speed_ref, energy_out_ref), targets, sems)


def moved_together(sources, targets, sems):
    copies = [pltpu.make_async_copy(a, b, sems.at[n]) for n, (a, b) in enumerate(zip(sources, targets))]
    for copy in copies:
        copy.start()
    for copy in copies:
        copy.wait()


def pack_kernel(grid, layout, *refs):
    sources, out_ref, held, sems = refs[:5], refs[5], refs[6:11], refs[11]
    moved_together(sources, held, sems)
    x_ref, v_ref, flag_ref, pair_ref, send_ref = held
    out_ref[...] = jnp.zeros(out_ref.shape, jnp.float32)
    for c in range(3):
        out_ref[pl.ds(layout["positions"] + 8 * c, 8), :] = x_ref[c]
        out_ref[pl.ds(layout["velocities"] + 8 * c, 8), :] = v_ref[c]
    out_ref[pl.ds(layout["flags"], 7), :] = flag_ref[...].astype(jnp.float32)
    for side in range(2):
        for block in range(grid.blocks):
            row = layout["pairs"] + side * grid.blocks + block
            ids = pair_ref[pl.ds(side, 1), pl.ds(block * LANES, LANES)]
            out_ref[pl.ds(row, 1), :] = ids.astype(jnp.float32)
    out_ref[pl.ds(layout["sends"], 1), :] = send_ref[:, :LANES].astype(jnp.float32)
    rest = send_ref.shape[1] - LANES
    out_ref[pl.ds(layout["sends"] + 1, 1), pl.ds(0, rest)] = send_ref[:, LANES:].astype(jnp.float32)


def from_ahead(value, steps):
    names = [a for a, by in zip(("gx", "gy", "gz"), steps) if by]
    if not names:
        return value
    counts = [lax.axis_size(a) for a in names]
    pairs = []
    for target in np.ndindex(*counts):
        source = [(t + by) % n for t, by, n in zip(target, [s for s in steps if s], counts)]
        pairs.append(tuple(int(np.ravel_multi_index(p, counts)) for p in (source, target)))
    return lax.ppermute(value, tuple(names), pairs)


def replicated(grid, positions, velocities, send_list, pair_list, constraint_flags):
    clusters = positions.shape[2]
    heights = dict(positions=ROWS, velocities=ROWS, flags=8, pairs=2 * grid.blocks, sends=2)
    layout, row = {}, 0
    for name, height in heights.items():
        layout[name] = row
        row += height
    params = pltpu.CompilerParams(vmem_limit_bytes=VMEM_LIMIT)

    def call(kernel, shapes, scratch, *values, **specs):
        return pl.pallas_call(kernel, out_shape=shapes, scratch_shapes=scratch, compiler_params=params, **specs)(*values)

    anywhere = pl.BlockSpec(memory_space=pltpu.MemorySpace.HBM)
    given = (positions, velocities, constraint_flags, pair_list, send_list.reshape(1, -1))
    given = [pltpu.with_memory_space_constraint(value, pltpu.MemorySpace.HBM) for value in given]

    pack = call(
        functools.partial(pack_kernel, grid, layout),
        jax.ShapeDtypeStruct((row + -row % 8, LANES), jnp.float32),
        [pltpu.VMEM(value.shape, value.dtype) for value in given] + [pltpu.SemaphoreType.DMA((len(given),))],
        *given,
        in_specs=[anywhere] * len(given),
    )
    column = jnp.stack([from_ahead(pack, (0, j, 0)) for j in range(grid.gy)])
    near = jnp.concatenate([from_ahead(column, (i, 0, 0)) for i in range(grid.gx)], axis=0)
    far = from_ahead(near, (0, 0, 1))
    f32, i32, b16 = jnp.float32, jnp.int32, jnp.bfloat16
    n, rows = grid.lists, grid.domains * 8
    cube = jax.ShapeDtypeStruct((3, rows, LANES), f32)
    plane = jax.ShapeDtypeStruct((rows, LANES), f32)
    small = jax.ShapeDtypeStruct((8, LANES), f32)
    forces = jax.ShapeDtypeStruct((3 * rows + 8, LANES), f32)
    ids, weight, table = call(
        functools.partial(table_kernel, grid, layout["pairs"]),
        [
            jax.ShapeDtypeStruct((2, n, grid.padded, LANES), i32),
            jax.ShapeDtypeStruct((n, grid.padded, LANES), f32),
            jax.ShapeDtypeStruct((n, 3, grid.slots, LANES), b16),
        ],
        [pltpu.VMEM((LANES, grid.slots), b16), pltpu.VMEM((n, LANES, LANES), b16)],
        near,
    )
    zone_shapes = [
        jax.ShapeDtypeStruct((n, 8, LANES), i32),
        jax.ShapeDtypeStruct((n, len(zone_list), LANES, LANES), b16),
    ]
    scratch = [
        pltpu.VMEM((3, 3, 8, LANES), f32),
        pltpu.VMEM((3, 3, 8, LANES), f32),
        pltpu.VMEM((2 * grid.padded * ROWS, LANES), f32),
        pltpu.VMEM((2 * grid.padded * ROWS, LANES), f32),
        pltpu.VMEM((n, ROWS, 2 * LANES), f32),
        pltpu.VMEM((8, LANES), f32),
    ]
    x, v, rest, flags, index, zone, force = call(
        functools.partial(start_kernel, grid, layout),
        [cube, cube, plane, plane] + zone_shapes + [forces],
        scratch,
        near, far, ids, weight, table,
    )
    tables = (ids, weight, index, table, zone)
    energies = jnp.zeros((8, LANES), f32)
    for step in range(ITERS):
        got = [from_ahead(force, (0, 0, by)) for by in range(1, grid.gz)]
        x, v, energies, force = call(
            functools.partial(step_kernel, grid, step),
            [cube, cube, small, forces],
            scratch,
            x, v, rest, flags, *tables, energies, force, *got,
        )
    got = [from_ahead(force, (0, 0, by)) for by in range(1, grid.gz)]
    own = jax.ShapeDtypeStruct((3, 8, LANES), f32)
    shapes = [own, own, jax.ShapeDtypeStruct((2, ITERS), f32)]
    place, speed, energies = call(
        functools.partial(last_kernel, grid, 8 * clusters * grid.domains),
        shapes,
        [pltpu.VMEM(shape.shape, f32) for shape in shapes] + [pltpu.SemaphoreType.DMA((len(shapes),))],
        x, v, energies, force, *got,
        out_specs=[anywhere] * len(shapes),
    )
    return (place, speed, energies.T)


def can_replicate(grid, positions, send_list, pair_list):
    return (
        grid.domains <= MAX_REPLICATED
        and grid.lists % 2 == 0
        and grid.gz == 2
        and 2 * grid.padded <= LANES
        and positions.shape[2] == LANES
        and zone_sizes()[0] == LANES
        and pair_list.shape[1] % LANES == 0
        and sum(zone_sizes()) == send_list.shape[0]
        and send_list.shape[0] - LANES < LANES
    )


VMEM_LIMIT = 16 * 1024 * 1024


def solution(mesh):
    def on_any(positions, velocities, send_list, pair_list, constraint_flags):
        grid = Grid(mesh, pair_list.shape[1], send_list.shape[0])
        if can_replicate(grid, positions, send_list, pair_list):
            return replicated(grid, positions, velocities, send_list, pair_list, constraint_flags)
        return on_device(positions, velocities, send_list, pair_list, constraint_flags)

    return jax.shard_map(
        on_any,
        mesh=mesh,
        in_specs=(
            P(None, None, ("runs", "gx", "gy", "gz")),
            P(None, None, ("runs", "gx", "gy", "gz")),
            P(("runs", "gx", "gy", "gz")),
            P(None, ("runs", "gx", "gy", "gz")),
            P(None, ("runs", "gx", "gy", "gz")),
        ),
        out_specs=(
            P(None, None, ("runs", "gx", "gy", "gz")),
            P(None, None, ("runs", "gx", "gy", "gz")),
            P("runs", None),
        ),
        check_vma=False,
    )
```

```python
import functools

import jax
import jax.numpy as jnp
import numpy as np
from jax import lax
from jax.experimental import pallas as pl
from jax.experimental.pallas import tpu as pltpu
from jax.sharding import PartitionSpec as P

CX = 1
CY = 8
CZ = 16
ITERS = 3
NORDER = 4


time_step = 0.02
strength = 2.0
root_half = 0.7071067811865476
zone_list = ((1, 0, 0), (0, 1, 0), (0, 0, 1), (1, 1, 0), (1, 0, 1), (0, 1, 1), (1, 1, 1))


def from_behind(value, axis, by):
    count = lax.axis_size(axis)
    return lax.ppermute(value, axis, [(i, (i + by) % count) for i in range(count)])


def zone_sizes():
    return tuple(
        (
            (CX if direction[0] == 0 else 1)
            * (CY if direction[1] == 0 else 1)
            * (CZ if direction[2] == 0 else 1)
            for direction in zone_list
        )
    )


def split_blocks(packed, block_sizes):
    pieces = []
    position = 0
    for length in block_sizes:
        pieces.append(packed[:, :, position : position + length])
        position += length
    return pieces


def shell_offsets():
    block_sizes = zone_sizes()
    columns = []
    for number in range(7):
        direction = zone_list[number]
        column = np.array(
            [[direction[0] * CX], [direction[1] * CY], [direction[2] * CZ]], np.float32
        )
        columns.append(np.tile(column, (1, block_sizes[number])))
    return jnp.asarray(np.concatenate(columns, axis=1))[:, None, :]


def share_coords(coords, send_table):
    sizes_all = zone_sizes()
    chosen = jnp.dot(
        coords.reshape(24, -1), send_table, precision=lax.Precision.HIGHEST
    ).reshape(3, 8, -1)
    outgoing = split_blocks(chosen, sizes_all)
    along_y = from_behind(
        jnp.concatenate([outgoing[1], outgoing[3], outgoing[5], outgoing[6]], axis=2), "gy", -1
    )
    got_y = split_blocks(along_y, [sizes_all[1], sizes_all[3], sizes_all[5], sizes_all[6]])
    along_x = from_behind(
        jnp.concatenate([outgoing[0], outgoing[4], got_y[1], got_y[3]], axis=2), "gx", -1
    )
    got_x = split_blocks(along_x, [sizes_all[0], sizes_all[4], sizes_all[3], sizes_all[6]])
    along_z = from_behind(
        jnp.concatenate([outgoing[2], got_x[1], got_y[2], got_x[3]], axis=2), "gz", -1
    )
    got_z = split_blocks(along_z, [sizes_all[2], sizes_all[4], sizes_all[5], sizes_all[6]])
    received = [got_x[0], got_y[0], got_z[0], got_x[2], got_z[1], got_z[2], got_z[3]]
    return jnp.concatenate(received, axis=2) + shell_offsets()


def return_forces(halo_forces):
    sizes_all = zone_sizes()
    outgoing = split_blocks(halo_forces, sizes_all)
    along_z = from_behind(
        jnp.concatenate([outgoing[2], outgoing[4], outgoing[5], outgoing[6]], axis=2), "gz", 1
    )
    got_z = split_blocks(along_z, [sizes_all[2], sizes_all[4], sizes_all[5], sizes_all[6]])
    along_x = from_behind(
        jnp.concatenate([outgoing[0], outgoing[3], got_z[1], got_z[3]], axis=2), "gx", 1
    )
    got_x = split_blocks(along_x, [sizes_all[0], sizes_all[3], sizes_all[4], sizes_all[6]])
    settled = [got_x[0], got_z[0], got_x[2]]
    pending = [got_x[1], got_z[2], got_x[3]]
    along_y = from_behind(
        jnp.concatenate([outgoing[1], pending[0], pending[1], pending[2]], axis=2), "gy", 1
    )
    got_y = split_blocks(along_y, [sizes_all[1], sizes_all[3], sizes_all[5], sizes_all[6]])
    return jnp.concatenate(
        [settled[0], got_y[0], settled[1], got_y[1], settled[2], got_y[2], got_y[3]], axis=2
    )


def pair_tables(pair_list, extended_count):
    rows = lax.broadcasted_iota(jnp.int32, (extended_count, pair_list.shape[1]), 0)
    first_table = (rows == pair_list[0][None, :]).astype(jnp.float32)
    second_table = (rows == pair_list[1][None, :]).astype(jnp.float32)
    return (first_table, second_table)


def domain_forces(extended, pair_list, tables):
    extended_count = extended.shape[2]
    slot_count = pair_list.shape[1]
    first_ids = pair_list[0]
    second_ids = pair_list[1]
    flat = extended.reshape(24, extended_count)
    first_coords = jnp.dot(flat, tables[0], precision=lax.Precision.HIGHEST).reshape(
        3, 8, slot_count
    )
    second_coords = jnp.dot(flat, tables[1], precision=lax.Precision.HIGHEST).reshape(
        3, 8, slot_count
    )
    separation = first_coords[:, :, None, :] - second_coords[:, None, :, :]
    scaled = jnp.sum(separation * separation, axis=0)
    intersect = jnp.maximum(1.0 - scaled, 0.0)
    bead_row = lax.broadcasted_iota(jnp.int32, (8, 8, 1), 0)
    bead_column = lax.broadcasted_iota(jnp.int32, (8, 8, 1), 1)
    self_pair = (first_ids == second_ids)[None, None, :]
    usable = (first_ids < extended_count - 1)[None, None, :]
    weight = (jnp.where(self_pair, bead_row < bead_column, True) & usable).astype(jnp.float32)
    energy = strength * jnp.sum(weight * intersect * intersect * intersect)
    magnitude = 6.0 * strength * weight * intersect * intersect
    pushing = magnitude[None] * separation
    on_first = jnp.sum(pushing, axis=2).reshape(24, slot_count)
    on_second = (-jnp.sum(pushing, axis=1)).reshape(24, slot_count)
    contract = (((1,), (1,)), ((), ()))
    forces = lax.dot_general(on_first, tables[0], contract, precision=lax.Precision.HIGHEST)
    forces = forces + lax.dot_general(
        on_second, tables[1], contract, precision=lax.Precision.HIGHEST
    )
    return (forces.reshape(3, 8, extended_count), energy)


def local_forces(coords, send_table, pair_list, tables):
    halo_coords = share_coords(coords, send_table)
    dummy_cluster = jnp.zeros((3, 8, 1), jnp.float32)
    extended = jnp.concatenate([coords, halo_coords, dummy_cluster], axis=2)
    forces, energy = domain_forces(extended, pair_list, tables)
    cluster_count = coords.shape[2]
    returned = return_forces(forces[:, :, cluster_count : cluster_count + send_table.shape[1]])
    contract = (((1,), (1,)), ((), ()))
    added = lax.dot_general(
        returned.reshape(24, -1), send_table, contract, precision=lax.Precision.HIGHEST
    )
    home_forces = forces[:, :, :cluster_count] + added.reshape(3, 8, -1)
    return (home_forces, energy)


def link_vectors(coords):
    return coords[:, :-1, :] - coords[:, 1:, :]


def link_lengths(coords):
    vectors = link_vectors(coords)
    return jnp.sqrt(jnp.sum(vectors * vectors, axis=0))


def expand(coupling, source):
    coupling_down = jnp.pad(coupling, ((1, 0), (0, 0)))
    coupling_up = jnp.pad(coupling, ((0, 1), (0, 0)))
    series = source
    result = source
    for _ in range(NORDER):
        series = (
            coupling_down * jnp.pad(series, ((1, 0), (0, 0)))[:-1]
            + coupling_up * jnp.pad(series, ((0, 1), (0, 0)))[1:]
        )
        result = result + series
    return result


def apply_links(coords, directions, solution):
    shifts = directions * (root_half * solution)[None]
    return (
        coords
        - jnp.pad(shifts, ((0, 0), (0, 1), (0, 0)))
        + jnp.pad(shifts, ((0, 0), (1, 0), (0, 0)))
    )


def constrain(previous, updated, rest_length, link_flags):
    old_vectors = link_vectors(previous)
    directions = (
        old_vectors / jnp.maximum(jnp.sqrt(jnp.sum(old_vectors * old_vectors, axis=0)), 0.2)[None]
    )
    coupling = (
        0.5
        * jnp.sum(directions[:, :-1] * directions[:, 1:], axis=0)
        * link_flags[:-1]
        * link_flags[1:]
    )
    projected = jnp.sum(directions * link_vectors(updated), axis=0)
    solution = expand(coupling, link_flags * root_half * (projected - rest_length))
    updated = apply_links(updated, directions, solution)
    vectors = link_vectors(updated)
    squared = jnp.sum(vectors * vectors, axis=0)
    target = jnp.sqrt(
        jnp.maximum(2.0 * rest_length * rest_length - squared, 0.25 * rest_length * rest_length)
    )
    solution = expand(coupling, link_flags * root_half * (rest_length - target))
    updated = apply_links(updated, directions, solution)
    return updated


def total_over(value, axis):
    count = lax.axis_size(axis)
    if count > 4:
        return lax.psum(value, axis)
    total = value
    for by in range(1, count):
        total = total + from_behind(value, axis, by)
    return total


def on_device(positions, velocities, send_list, pair_list, constraint_flags):
    link_flags = constraint_flags.astype(jnp.float32)
    rest_length = link_lengths(positions)
    bead_total = 8 * positions.shape[2] * lax.axis_size(("gx", "gy", "gz"))
    tables = pair_tables(pair_list, positions.shape[2] + send_list.shape[0] + 1)
    owned = lax.broadcasted_iota(jnp.int32, (positions.shape[2], send_list.shape[0]), 0)
    send_table = (owned == send_list[None, :]).astype(jnp.float32)
    forces, potential = local_forces(positions, send_table, pair_list, tables)
    energy_rows = []
    for _ in range(ITERS):
        half_speed = velocities + 0.5 * time_step * forces
        updated = constrain(positions, positions + time_step * half_speed, rest_length, link_flags)
        half_speed = (updated - positions) / time_step
        forces, potential = local_forces(updated, send_table, pair_list, tables)
        velocities = half_speed + 0.5 * time_step * forces
        positions = updated
        kinetic = 0.5 * jnp.sum(velocities * velocities)
        energy_rows.append(jnp.stack([potential, kinetic]))
    energies = jnp.stack(energy_rows)
    for axis in ("gz", "gy", "gx"):
        energies = total_over(energies, axis)
    return (positions, velocities, energies / bead_total)


LANES = 128
ROWS = 24
MAX_REPLICATED = 16


def split_rows(value):
    high = value.astype(jnp.bfloat16).astype(jnp.float32)
    return jnp.concatenate([high, value - high], axis=0).astype(jnp.bfloat16)


def joined(value):
    return value[:ROWS] + value[ROWS:]


class Grid:
    def __init__(self, mesh, slot_count, halo_count):
        self.gx, self.gy, self.gz = (mesh.shape[a] for a in ("gx", "gy", "gz"))
        self.domains = self.gx * self.gy * self.gz
        self.lists = self.gx * self.gy
        self.blocks = slot_count // LANES
        self.padded = (self.blocks + 7) // 8 * 8
        self.dummy = LANES + halo_count
        self.slots = 2 * self.blocks * LANES
        sizes = zone_sizes()
        self.zones = []
        start = 0
        for direction, size in zip(zone_list[1:], sizes[1:]):
            self.zones.append((direction, start, start + size))
            start += size

    def domain(self, i, j, direction):
        i = lax.rem(i + direction[0], self.gx) if not isinstance(i, int) else (i + direction[0]) % self.gx
        j = lax.rem(j + direction[1], self.gy) if not isinstance(j, int) else (j + direction[1]) % self.gy
        return (i * self.gy + j) * self.gz + direction[2] % self.gz

    def rows_of(self, i, j, direction):
        row = self.domain(i, j, direction) * 8
        return pl.ds(row if isinstance(row, int) else pl.multiple_of(row, 8), 8)


def lanes_of(shape):
    return lax.broadcasted_iota(jnp.int32, shape, 1)


def take_lanes(source, index):
    return jnp.take_along_axis(source, index, axis=1, mode="promise_in_bounds")


def rounded_iota(shape, dimension, start=0):
    return (lax.broadcasted_iota(jnp.int32, shape, dimension) + start).astype(jnp.float32).astype(jnp.bfloat16)


def table_kernel(grid, pair_row, first, near_ref, *refs):
    ids_ref, weight_ref, table_ref, spread_ref, turned_ref = refs[-5:]
    blocks = grid.blocks
    count = near_ref.shape[0] if first == 0 else grid.lists - first
    square = (LANES, LANES)
    codes_of = (rounded_iota(square, 1), rounded_iota(square, 1, LANES), -rounded_iota(square, 1, 1))
    one, zero = jnp.ones(square, jnp.bfloat16), jnp.zeros(square, jnp.bfloat16)
    row = rounded_iota(square, 0)
    for at in range(2 * blocks):
        place = at // blocks * grid.padded + at % blocks
        spread_ref[:, pl.ds(at * LANES, LANES)] = jnp.where(row == place, one, zero)
    for number in range(first, first + count):
        sides = []
        for side in range(2):
            ids = near_ref[number, pl.ds(pair_row + side * blocks, blocks), :]
            fill = jnp.full((grid.padded - blocks, LANES), float(grid.dummy), jnp.float32)
            sides.append(jnp.concatenate([ids, fill], axis=0) if grid.padded > blocks else ids)
            ids_ref[side, number] = sides[side].astype(jnp.int32)
        usable = jnp.where(sides[0] < float(grid.dummy), 1.0, 0.0)
        weight_ref[number] = jnp.where(sides[0] == sides[1], 0.5, 1.0) * usable
        codes = jnp.concatenate(sides, axis=0)
        codes = jnp.where(codes < 2.0 * LANES, codes, 2.0 * LANES - 1.0 - codes)
        empty = jnp.zeros((LANES - 2 * grid.padded, LANES), jnp.float32)
        turned_ref[number] = jnp.transpose(jnp.concatenate([codes, empty], axis=0)).astype(jnp.bfloat16)

    def one_list(number, carry):
        wide = jnp.dot(turned_ref[number], spread_ref[...], preferred_element_type=jnp.float32)
        for at in range(2 * blocks):
            column = wide[:, at * LANES : (at + 1) * LANES].astype(jnp.bfloat16)
            for part, code in enumerate(codes_of):
                hot = jnp.where(column == code, one, zero)
                table_ref[number, part, pl.ds(at * LANES, LANES), :] = hot
        return carry

    lax.fori_loop(first, first + count, one_list, 0)


def build_zones(grid, near_ref, far_ref, send_row, index_ref, zone_ref):
    square = (LANES, LANES)
    lane = lanes_of((1, LANES))
    own_code = rounded_iota(square, 1)
    slot = rounded_iota(square, 0)
    one, zero = jnp.ones(square, jnp.bfloat16), jnp.zeros(square, jnp.bfloat16)

    def send_of(number, row):
        source = near_ref if number % grid.gz == 0 else far_ref
        return source[number // grid.gz, pl.ds(send_row + row, 1), :]

    for number in range(grid.lists):
        i, j = number // grid.gy, number % grid.gy
        to_x = send_of(grid.domain(i, j, zone_list[0]), 0)
        rest = jnp.zeros((1, LANES), jnp.float32)
        for direction, start, stop in grid.zones:
            row = send_of(grid.domain(i, j, direction), 1)
            rest = jnp.where((lane >= start) & (lane < stop), row, rest)
        both = jnp.concatenate([to_x, rest] + [jnp.zeros((6, LANES), jnp.float32)], axis=0)
        index_ref[number] = both.astype(jnp.int32)

    def one_list(number, carry):
        turned = jnp.transpose(index_ref[number].astype(jnp.float32))
        column = jnp.broadcast_to(turned[:, 0:1], square).astype(jnp.bfloat16)
        zone_ref[number, 0] = jnp.where(column == own_code, one, zero)
        column = jnp.broadcast_to(turned[:, 1:2], square).astype(jnp.bfloat16)
        for part, (direction, start, stop) in enumerate(grid.zones):
            here = (column == own_code) & (slot >= start) & (slot < stop)
            zone_ref[number, part + 1] = jnp.where(here, one, zero)
        return carry

    lax.fori_loop(0, grid.lists, one_list, 0)


def gather_and_push(grid, number, x_ref, ids_ref, weight_ref, index_ref, ext_ref, push_ref, energy_ref):
    i, j = lax.div(number, grid.gy), lax.rem(number, grid.gy)
    lane = lanes_of((8, LANES))
    cell = (CX, CY, CZ)
    to_x = jnp.broadcast_to(index_ref[number, pl.ds(0, 1), :], (8, LANES))
    rest = jnp.broadcast_to(index_ref[number, pl.ds(1, 1), :], (8, LANES))
    for c in range(3):
        ext_ref[c, 0] = x_ref[c, grid.rows_of(i, j, (0, 0, 0)), :]
        shift = float(zone_list[0][c] * cell[c])
        ext_ref[c, 1] = take_lanes(x_ref[c, grid.rows_of(i, j, zone_list[0]), :], to_x) + shift
        value = jnp.zeros((8, LANES), jnp.float32)
        for direction, start, stop in grid.zones:
            shift = float(direction[c] * cell[c])
            got = take_lanes(x_ref[c, grid.rows_of(i, j, direction), :], rest) + shift
            value = jnp.where((lane >= start) & (lane < stop), got, value)
        ext_ref[c, 2] = value
    for group in range(grid.padded // 8):
        sides = []
        for side in range(2):
            ids = ids_ref[side, number, pl.ds(8 * group, 8), :]
            low = ids & (LANES - 1)
            in_own = ids < LANES
            in_first = ids < 2 * LANES
            coords = []
            for c in range(3):
                line = []
                for bead in range(8):
                    a, b, d = (
                        take_lanes(jnp.broadcast_to(ext_ref[c, part, pl.ds(bead, 1), :], (8, LANES)), low)
                        for part in range(3)
                    )
                    line.append(jnp.where(in_own, a, jnp.where(in_first, b, d)))
                coords.append(line)
            sides.append(coords)
        weight = weight_ref[number, pl.ds(8 * group, 8), :]
        scale = weight * (6.0 * strength)
        energy = None
        partial = [None] * 8
        for half in range(2):
            beads = range(4 * half, 4 * half + 4)
            second = {l: [sides[1][c][l] for c in range(3)] for l in beads}
            on_second = {l: None for l in beads}
            for k in range(8):
                on_first = partial[k]
                first = [sides[0][c][k] for c in range(3)]
                for l in beads:
                    apart = [first[c] - second[l][c] for c in range(3)]
                    scaled = apart[0] * apart[0] + apart[1] * apart[1] + apart[2] * apart[2]
                    intersect = jnp.maximum(1.0 - scaled, 0.0)
                    square = intersect * intersect
                    cube = square * intersect
                    energy = cube if energy is None else energy + cube
                    pushing = [square * apart[c] for c in range(3)]
                    on_first = pushing if on_first is None else [on_first[c] + pushing[c] for c in range(3)]
                    on_second[l] = pushing if k == 0 else [on_second[l][c] + pushing[c] for c in range(3)]
                partial[k] = on_first
                if half == 1:
                    for c in range(3):
                        row = (8 * group) * ROWS + c * 8 + k
                        push_ref[pl.ds(row, 8, stride=ROWS), :] = on_first[c] * scale
            for c in range(3):
                for l in beads:
                    row = (grid.padded + 8 * group) * ROWS + c * 8 + l
                    push_ref[pl.ds(row, 8, stride=ROWS), :] = on_second[l][c] * (-scale)
        own_beads = jnp.where(weight == 0.5, 8.0, 0.0)
        energy_ref[...] += strength * weight * (energy - own_beads)


def scatter(grid, number, push_ref, table_ref, force_ref, halo_ref):
    pieces = []
    for side in range(2):
        for block in range(grid.blocks):
            pieces.append(push_ref[pl.ds((side * grid.padded + block) * ROWS, ROWS), :])
    pushes = split_rows(jnp.concatenate(pieces, axis=1))
    table = jnp.concatenate([table_ref[number, part] for part in range(3)], axis=1)
    sums = joined(jnp.dot(pushes, table, preferred_element_type=jnp.float32))
    row = pl.multiple_of(number * grid.gz * 8, 8)
    for c in range(3):
        force_ref[pl.ds(c * grid.domains * 8 + row, 8), :] = sums[8 * c : 8 * c + 8, :LANES]
    halo_ref[number] = sums[:, LANES:]


def pair_forces(grid, x_ref, tables, force_ref, scratch):
    ids_ref, weight_ref, index_ref, table_ref, zone_ref = tables
    ext_a, ext_b, push_a, push_b, halo_ref, energy_ref = scratch
    force_ref[...] = jnp.zeros(force_ref.shape, jnp.float32)
    energy_ref[...] = jnp.zeros((8, LANES), jnp.float32)

    def forward(number, ext_ref, push_ref):
        gather_and_push(grid, number, x_ref, ids_ref, weight_ref, index_ref, ext_ref, push_ref, energy_ref)

    def back(number, push_ref):
        scatter(grid, number, push_ref, table_ref, force_ref, halo_ref)

    forward(0, ext_a, push_a)

    def two(m, carry):
        back(2 * m, push_a)
        forward(2 * m + 1, ext_b, push_b)
        back(2 * m + 1, push_b)
        forward(2 * m + 2, ext_a, push_a)
        return carry

    lax.fori_loop(0, grid.lists // 2 - 1, two, 0)
    back(grid.lists - 2, push_a)
    forward(grid.lists - 1, ext_b, push_b)
    back(grid.lists - 1, push_b)
    for number in range(grid.lists):
        i, j = number // grid.gy, number % grid.gy
        halo = halo_ref[number]
        to_x = joined(
            jnp.dot(split_rows(halo[:, :LANES]), zone_ref[number, 0], preferred_element_type=jnp.float32)
        )
        rest = joined(
            jnp.dot(
                split_rows(halo[:, LANES:]),
                jnp.concatenate([zone_ref[number, part + 1] for part in range(len(grid.zones))], axis=1),
                preferred_element_type=jnp.float32,
            )
        )
        targets = [(zone_list[0], to_x)]
        for part, (direction, start, stop) in enumerate(grid.zones):
            targets.append((direction, rest[:, part * LANES : (part + 1) * LANES]))
        for direction, value in targets:
            row = grid.domain(i, j, direction) * 8
            for c in range(3):
                force_ref[pl.ds(c * grid.domains * 8 + row, 8), :] += value[8 * c : 8 * c + 8]
    force_ref[pl.ds(3 * grid.domains * 8, 8), :] = energy_ref[...]


def start_kernel(grid, layout, near_ref, far_ref, ids_ref, weight_ref, table_ref, *refs):
    x_ref, v_ref, rest_ref, flag_ref, index_ref, zone_ref, force_ref = refs[:7]
    scratch = refs[7:]
    for number in range(grid.domains):
        source = near_ref if number % grid.gz == 0 else far_ref
        at = number // grid.gz
        rows = pl.ds(number * 8, 8)
        for c in range(3):
            x_ref[c, rows, :] = source[at, pl.ds(layout["positions"] + 8 * c, 8), :]
            v_ref[c, rows, :] = source[at, pl.ds(layout["velocities"] + 8 * c, 8), :]
        flag_ref[rows, :] = source[at, pl.ds(layout["flags"], 8), :]
    rest_ref[...] = link_length([x_ref[c] for c in range(3)])
    build_zones(grid, near_ref, far_ref, layout["sends"], index_ref, zone_ref)
    pair_forces(grid, x_ref, (ids_ref, weight_ref, index_ref, table_ref, zone_ref), force_ref, scratch)


def up(value):
    return pltpu.roll(value, value.shape[0] - 1, 0)


def down(value):
    return pltpu.roll(value, 1, 0)


def dot3(a, b):
    return a[0] * b[0] + a[1] * b[1] + a[2] * b[2]


def links_of(x):
    return [c - up(c) for c in x]


def link_length(x):
    vectors = links_of(x)
    return jnp.sqrt(dot3(vectors, vectors))


def expand_rows(coupling, before, source):
    series = source
    result = source
    for _ in range(NORDER):
        series = before * down(series) + coupling * up(series)
        result = result + series
    return result


def apply_rows(x, directions, solution):
    moved = []
    for c in range(3):
        shift = directions[c] * (root_half * solution)
        moved.append(x[c] - shift + down(shift))
    return moved


def constrain_rows(previous, updated, rest, flags):
    old = links_of(previous)
    length = jnp.maximum(jnp.sqrt(dot3(old, old)), 0.2)
    directions = [c / length for c in old]
    coupling = 0.5 * dot3(directions, [up(c) for c in directions]) * flags * up(flags)
    before = down(coupling)
    projected = dot3(directions, links_of(updated))
    solution = expand_rows(coupling, before, flags * (root_half * (projected - rest)))
    updated = apply_rows(updated, directions, solution)
    vectors = links_of(updated)
    squared = dot3(vectors, vectors)
    target = jnp.sqrt(jnp.maximum(2.0 * rest * rest - squared, 0.25 * rest * rest))
    solution = expand_rows(coupling, before, flags * (root_half * (rest - target)))
    return apply_rows(updated, directions, solution)


def total_force(grid, own_ref, got_refs):
    size = grid.domains * 8
    total = []
    for c in range(3):
        pieces = []
        for number in range(grid.domains):
            base, k = number // grid.gz * grid.gz, number % grid.gz
            value = own_ref[pl.ds(c * size + number * 8, 8), :]
            for by, ref in enumerate(got_refs, 1):
                value = value + ref[pl.ds(c * size + (base + (k - by) % grid.gz) * 8, 8), :]
            pieces.append(value)
        total.append(jnp.concatenate(pieces, axis=0))
    return total


def energy_row(grid, own_ref, got_refs, v, step, previous):
    rows = pl.ds(3 * grid.domains * 8, 8)
    potential = own_ref[rows, :]
    for ref in got_refs:
        potential = potential + ref[rows, :]
    kinetic = 0.5 * dot3(v, v)
    here = lanes_of((8, LANES)) == step
    row = lax.broadcasted_iota(jnp.int32, (8, LANES), 0)
    previous = jnp.where(here & (row == 0), jnp.sum(potential), previous)
    return jnp.where(here & (row == 1), jnp.sum(kinetic), previous)


def step_kernel(grid, step, x_ref, v_ref, rest_ref, flag_ref, ids_ref, weight_ref, index_ref, table_ref, zone_ref, energies_ref, own_ref, *refs):
    got_refs, refs = refs[: grid.gz - 1], refs[grid.gz - 1 :]
    moved_ref, half_ref, energy_out_ref, force_ref = refs[:4]
    scratch = refs[4:]
    force = total_force(grid, own_ref, got_refs)
    x = [x_ref[c] for c in range(3)]
    v = [v_ref[c] for c in range(3)]
    if step > 0:
        v = [v[c] + (0.5 * time_step) * force[c] for c in range(3)]
        energy_out_ref[...] = energy_row(grid, own_ref, got_refs, v, step - 1, energies_ref[...])
    else:
        energy_out_ref[...] = energies_ref[...]
    half = [v[c] + (0.5 * time_step) * force[c] for c in range(3)]
    moved = constrain_rows(x, [x[c] + time_step * half[c] for c in range(3)], rest_ref[...], flag_ref[...])
    for c in range(3):
        moved_ref[c] = moved[c]
        half_ref[c] = (moved[c] - x[c]) / time_step
    pair_forces(grid, moved_ref, (ids_ref, weight_ref, index_ref, table_ref, zone_ref), force_ref, scratch)


def last_kernel(grid, bead_total, x_ref, v_ref, energies_ref, own_ref, *refs):
    got_refs, refs = refs[: grid.gz - 1], refs[grid.gz - 1 :]
    targets, (place_ref, speed_ref, energy_out_ref), sems = refs[:3], refs[3:6], refs[6]
    force = total_force(grid, own_ref, got_refs)
    v = [v_ref[c] + (0.5 * time_step) * force[c] for c in range(3)]
    for c in range(3):
        place_ref[c] = x_ref[c, pl.ds(0, 8), :]
        speed_ref[c] = v[c][:8]
    energies = energy_row(grid, own_ref, got_refs, v, ITERS - 1, energies_ref[...])
    energy_out_ref[...] = energies[:2, :ITERS] / bead_total
    moved_together((place_ref, speed_ref, energy_out_ref), targets, sems)


def moved_together(sources, targets, sems):
    copies = [pltpu.make_async_copy(a, b, sems.at[n]) for n, (a, b) in enumerate(zip(sources, targets))]
    for copy in copies:
        copy.start()
    for copy in copies:
        copy.wait()


def pack_kernel(grid, layout, *refs):
    sources, out_ref, held, sems = refs[:5], refs[5], refs[6:11], refs[11]
    moved_together(sources, held, sems)
    x_ref, v_ref, flag_ref, pair_ref, send_ref = held
    out_ref[...] = jnp.zeros(out_ref.shape, jnp.float32)
    for c in range(3):
        out_ref[pl.ds(layout["positions"] + 8 * c, 8), :] = x_ref[c]
        out_ref[pl.ds(layout["velocities"] + 8 * c, 8), :] = v_ref[c]
    out_ref[pl.ds(layout["flags"], 7), :] = flag_ref[...].astype(jnp.float32)
    for side in range(2):
        for block in range(grid.blocks):
            row = layout["pairs"] + side * grid.blocks + block
            ids = pair_ref[pl.ds(side, 1), pl.ds(block * LANES, LANES)]
            out_ref[pl.ds(row, 1), :] = ids.astype(jnp.float32)
    out_ref[pl.ds(layout["sends"], 1), :] = send_ref[:, :LANES].astype(jnp.float32)
    rest = send_ref.shape[1] - LANES
    out_ref[pl.ds(layout["sends"] + 1, 1), pl.ds(0, rest)] = send_ref[:, LANES:].astype(jnp.float32)


def from_ahead(value, steps):
    names = [a for a, by in zip(("gx", "gy", "gz"), steps) if by]
    if not names:
        return value
    counts = [lax.axis_size(a) for a in names]
    pairs = []
    for target in np.ndindex(*counts):
        source = [(t + by) % n for t, by, n in zip(target, [s for s in steps if s], counts)]
        pairs.append(tuple(int(np.ravel_multi_index(p, counts)) for p in (source, target)))
    return lax.ppermute(value, tuple(names), pairs)


def replicated(grid, positions, velocities, send_list, pair_list, constraint_flags):
    clusters = positions.shape[2]
    heights = dict(positions=ROWS, velocities=ROWS, flags=8, pairs=2 * grid.blocks, sends=2)
    layout, row = {}, 0
    for name, height in heights.items():
        layout[name] = row
        row += height
    params = pltpu.CompilerParams(vmem_limit_bytes=VMEM_LIMIT)

    def call(kernel, shapes, scratch, *values, **specs):
        return pl.pallas_call(kernel, out_shape=shapes, scratch_shapes=scratch, compiler_params=params, **specs)(*values)

    anywhere = pl.BlockSpec(memory_space=pltpu.MemorySpace.HBM)
    whole = pl.BlockSpec(memory_space=pltpu.MemorySpace.VMEM)
    given = (positions, velocities, constraint_flags, pair_list, send_list.reshape(1, -1))
    given = [pltpu.with_memory_space_constraint(value, pltpu.MemorySpace.HBM) for value in given]

    pack = call(
        functools.partial(pack_kernel, grid, layout),
        jax.ShapeDtypeStruct((row + -row % 8, LANES), jnp.float32),
        [pltpu.VMEM(value.shape, value.dtype) for value in given] + [pltpu.SemaphoreType.DMA((len(given),))],
        *given,
        in_specs=[anywhere] * len(given),
    )
    column = jnp.stack([from_ahead(pack, (0, j, 0)) for j in range(grid.gy)])
    f32, i32, b16 = jnp.float32, jnp.int32, jnp.bfloat16
    n, rows = grid.lists, grid.domains * 8
    cube = jax.ShapeDtypeStruct((3, rows, LANES), f32)
    plane = jax.ShapeDtypeStruct((rows, LANES), f32)
    small = jax.ShapeDtypeStruct((8, LANES), f32)
    forces = jax.ShapeDtypeStruct((3 * rows + 8, LANES), f32)
    shapes = [
        jax.ShapeDtypeStruct((2, n, grid.padded, LANES), i32),
        jax.ShapeDtypeStruct((n, grid.padded, LANES), f32),
        jax.ShapeDtypeStruct((n, 3, grid.slots, LANES), b16),
    ]
    room = [pltpu.VMEM((LANES, grid.slots), b16), pltpu.VMEM((n, LANES, LANES), b16)]
    begun = call(functools.partial(table_kernel, grid, layout["pairs"], 0), shapes, room, column)
    ahead = [column]
    for i in range(1, grid.gx):
        ahead.append(from_ahead(column, (i, 0, 0)))
    ahead, begun = lax.optimization_barrier((ahead, begun))
    near = jnp.concatenate(ahead, axis=0)
    far = from_ahead(near, (0, 0, 1))
    ids, weight, table = call(
        functools.partial(table_kernel, grid, layout["pairs"], grid.gy),
        shapes,
        room,
        near, *begun,
        input_output_aliases={1: 0, 2: 1, 3: 2},
        in_specs=[whole] + [pl.BlockSpec(memory_space=pl.ANY)] * 3,
    )
    zone_shapes = [
        jax.ShapeDtypeStruct((n, 8, LANES), i32),
        jax.ShapeDtypeStruct((n, len(zone_list), LANES, LANES), b16),
    ]
    scratch = [
        pltpu.VMEM((3, 3, 8, LANES), f32),
        pltpu.VMEM((3, 3, 8, LANES), f32),
        pltpu.VMEM((2 * grid.padded * ROWS, LANES), f32),
        pltpu.VMEM((2 * grid.padded * ROWS, LANES), f32),
        pltpu.VMEM((n, ROWS, 2 * LANES), f32),
        pltpu.VMEM((8, LANES), f32),
    ]
    x, v, rest, flags, index, zone, force = call(
        functools.partial(start_kernel, grid, layout),
        [cube, cube, plane, plane] + zone_shapes + [forces],
        scratch,
        near, far, ids, weight, table,
    )
    tables = (ids, weight, index, table, zone)
    energies = jnp.zeros((8, LANES), f32)
    for step in range(ITERS):
        got = [from_ahead(force, (0, 0, by)) for by in range(1, grid.gz)]
        x, v, energies, force = call(
            functools.partial(step_kernel, grid, step),
            [cube, cube, small, forces],
            scratch,
            x, v, rest, flags, *tables, energies, force, *got,
        )
    got = [from_ahead(force, (0, 0, by)) for by in range(1, grid.gz)]
    own = jax.ShapeDtypeStruct((3, 8, LANES), f32)
    shapes = [own, own, jax.ShapeDtypeStruct((2, ITERS), f32)]
    place, speed, energies = call(
        functools.partial(last_kernel, grid, 8 * clusters * grid.domains),
        shapes,
        [pltpu.VMEM(shape.shape, f32) for shape in shapes] + [pltpu.SemaphoreType.DMA((len(shapes),))],
        x, v, energies, force, *got,
        out_specs=[anywhere] * len(shapes),
    )
    return (place, speed, energies.T)


def can_replicate(grid, positions, send_list, pair_list):
    return (
        grid.domains <= MAX_REPLICATED
        and grid.lists % 2 == 0
        and grid.gz == 2
        and grid.gx > 1
        and 2 * grid.padded <= LANES
        and positions.shape[2] == LANES
        and zone_sizes()[0] == LANES
        and pair_list.shape[1] % LANES == 0
        and sum(zone_sizes()) == send_list.shape[0]
        and send_list.shape[0] - LANES < LANES
    )


VMEM_LIMIT = 16 * 1024 * 1024


def solution(mesh):
    def on_any(positions, velocities, send_list, pair_list, constraint_flags):
        grid = Grid(mesh, pair_list.shape[1], send_list.shape[0])
        if can_replicate(grid, positions, send_list, pair_list):
            return replicated(grid, positions, velocities, send_list, pair_list, constraint_flags)
        return on_device(positions, velocities, send_list, pair_list, constraint_flags)

    return jax.shard_map(
        on_any,
        mesh=mesh,
        in_specs=(
            P(None, None, ("runs", "gx", "gy", "gz")),
            P(None, None, ("runs", "gx", "gy", "gz")),
            P(("runs", "gx", "gy", "gz")),
            P(None, ("runs", "gx", "gy", "gz")),
            P(None, ("runs", "gx", "gy", "gz")),
        ),
        out_specs=(
            P(None, None, ("runs", "gx", "gy", "gz")),
            P(None, None, ("runs", "gx", "gy", "gz")),
            P("runs", None),
        ),
        check_vma=False,
    )
```
